128 devices in a mesh: section: 8 (over x, y_lo), dp: 16 (over z, y_hi, core).
Axes of the slice: x: 4, y: 4 (y_hi: 2, y_lo: 2; y = y_hi * 2 + y_lo), z: 4, core: 2. Of those that a mesh axis runs over, the one named last changes fastest.
Arguments:
- inputs: bfloat16 [32, 128, 3072], P('dp'), may hold values from -6 to 6
- sample_ids: int32 [16, 2], P('dp'), may hold values from 0 to 1, each once within a row
- stored: bfloat16 [8, 2, 32, 128, 3072], P('section', None, 'dp'), may hold values from -4 to 4, as said below
- weight: bfloat16 [8, 3072, 3072], P('section'), may hold values from -0.109375 to 0.109375
- norm_gain: float32 [8, 3072], P('section'), may hold values from 0.1 to 1.9
Outputs:
- section_outputs: bfloat16 [8, 32, 128, 3072], P('section', 'dp')
- weight_grads: bfloat16 [8, 3072, 3072], P('section', 'dp')
The draws below stay inside these ranges and needn't reach their ends.
Inputs may be any that keep to these rules, and one draw needn't show every extreme that they name: `sample_ids`: each row names each of the replica's 2 samples once. `stored`: copy 0 of section s equals copy 1 of section s - 1, and copy 0 of section 0 equals copy 1 of the last section.
All inputs are finite; a program needn't handle non-finite values.
Results may differ from the reference program's by a relative error of at most 0.024.
Values may be sent and summed in bfloat16 or wider, within the bound.
A program may use at most 192 MiB of HBM per device.

```python
import math
import jax
import jax.numpy as jnp
from jax import lax

D = 3072
TOK = 128
MB = 2
N_SECTION = 8
N_DP = 16


def draw_stored(key, part):
    full_shape = (N_SECTION, N_DP * MB, TOK, D)
    base_draw = jnp.clip(jax.random.normal(key, full_shape, jnp.float32), -4.0, 4.0)
    return jnp.stack([jnp.roll(base_draw, 1, axis=0), base_draw], axis=1).astype(jnp.bfloat16)


def level_of(key, extent, shards, smallest, high):
    def one(position, blocks):
        heights = jax.random.uniform(jax.random.fold_in(jax.random.fold_in(key, 6), position), (blocks,), jnp.float32, smallest / len(shards), high / len(shards))
        return jnp.repeat(jnp.exp(heights), extent[position] // blocks).reshape((-1,) + (1,) * (len(extent) - position - 1))

    factor_of = one(*shards[0])
    for cut in shards[1:]:
        factor_of = factor_of * one(*cut)
    return factor_of


def noise(rng, extent, deviation, limit, shards=(), kind=jnp.bfloat16):
    values = deviation * jax.random.normal(rng, extent, jnp.float32)
    if shards:
        values = values * level_of(rng, extent, shards, -0.22, 0.18)
    return jnp.clip(values, -limit, limit).astype(kind)


def setup_inputs(seed: int = 0) -> dict:
    keys = jax.random.split(jax.random.key(seed), 6)
    inputs = noise(keys[0], (N_DP * MB, TOK, D), 1.0, 6.0, ((0, 16),))
    sample_ids = jax.vmap(lambda own: jax.random.permutation(own, MB))(jax.random.split(keys[1], N_DP)).reshape((N_DP, MB)).astype(jnp.int32)
    stored = draw_stored(jax.random.fold_in(keys[5], 71), 0)
    weight = noise(keys[3], (N_SECTION, D, D), D ** -0.5, 0.109375, ((0, 8),))
    norm_gain = jnp.clip(1.0 + 0.18 * jax.random.normal(keys[4], (N_SECTION, D), jnp.float32), 0.1, 1.9)
    return {"inputs": inputs, "sample_ids": sample_ids, "stored": stored, "weight": weight, "norm_gain": norm_gain}


epsilon = 1e-05
delta_bound = 2.0

def activate(values):
    return jax.nn.gelu(values, approximate=False)

def normalize(state, norm_gain):
    average = lax.optimization_barrier(jnp.mean(state, axis=-1, keepdims=True))
    centred = state - average
    variance = lax.optimization_barrier(jnp.mean(centred * centred, axis=-1, keepdims=True))
    return centred * lax.rsqrt(variance + epsilon) * norm_gain

def reference(inputs, sample_ids, stored, weight, norm_gain):
    replica_base = jnp.arange(N_DP, dtype=jnp.int32)[:, None] * MB
    flat_ids = (replica_base + sample_ids.astype(jnp.int32)).reshape(-1).astype(jnp.int32)
    state = inputs.astype(jnp.float32)
    results = []
    stashed = []
    result = state
    for layer_num in range(N_SECTION):
        normed = normalize(state, norm_gain[layer_num]).astype(jnp.bfloat16)
        preact = jnp.dot(normed.reshape(-1, D), weight[layer_num], preferred_element_type=jnp.float32).reshape(state.shape)
        result = state + activate(preact)
        stashed.append((state, normed, preact))
        results.append(result.astype(jnp.bfloat16))
        if layer_num + 1 < N_SECTION:
            sent_copy = stored[layer_num, 1][flat_ids].astype(jnp.float32)
            kept_copy = stored[layer_num + 1, 0][flat_ids].astype(jnp.float32)
            clipped = jnp.clip(result - sent_copy, -delta_bound, delta_bound).astype(jnp.bfloat16)
            clipped = lax.optimization_barrier(clipped)
            state = kept_copy + clipped.astype(jnp.float32)
    loss_scale = 1.0 / math.sqrt(N_DP * MB * TOK)
    upstream = result * loss_scale
    weight_grads = [None] * N_SECTION

    def add_replica(total, operands):
        normed_rows, grad_rows = operands
        replica_sum = jnp.dot(normed_rows.T, grad_rows, preferred_element_type=jnp.float32).astype(jnp.bfloat16)
        replica_sum = lax.optimization_barrier(replica_sum)
        return (total + replica_sum.astype(jnp.float32), None)
    for layer_num in range(N_SECTION - 1, -1, -1):
        state, normed, preact = stashed[layer_num]
        grad_pre = jax.vjp(activate, preact)[1](upstream)[0].astype(jnp.bfloat16)
        normed_split = normed.reshape(N_DP, MB * TOK, D)
        grad_split = grad_pre.reshape(N_DP, MB * TOK, D)
        total, unused = lax.scan(add_replica, jnp.zeros((D, D), jnp.float32), (normed_split, grad_split))
        weight_grads[layer_num] = total.astype(jnp.bfloat16)
        grad_normed = jnp.dot(grad_pre.reshape(-1, D), weight[layer_num].T, preferred_element_type=jnp.float32).reshape(state.shape)
        gain_here = norm_gain[layer_num]
        grad_state = upstream + jax.vjp(lambda values: normalize(values, gain_here), state)[1](grad_normed)[0]
        sent = lax.optimization_barrier(grad_state.astype(jnp.bfloat16))
        upstream = sent.astype(jnp.float32)
    return (jnp.stack(results), jnp.stack(weight_grads))
```

```python
import functools
import math

import jax
import jax.numpy as jnp
from jax import lax
from jax.experimental import pallas as pl
from jax.experimental.pallas import tpu as pltpu
from jax.sharding import PartitionSpec as P

epsilon = 1e-05
delta_bound = 2.0
CHUNK = 32
PIECES = 4
MESH = pl.DeviceIdType.MESH
f32 = jnp.float32
bf16 = jnp.bfloat16
rsqrt2 = 1.0 / math.sqrt(2.0)
rsqrt2pi = 1.0 / math.sqrt(2.0 * math.pi)


def relay_kernel(
    scale,
    ids_ref, inputs_hbm, stored_hbm, w_hbm, gain_ref,
    out_hbm, normed_hbm, grad_hbm,
    w_v, base_v, keep_v, fin_v, clip_v, normed_v, pre_v, out_v, bin_v, bout_v, gp_v,
    acc_v, up_v, mu_v, rs_v,
    sem_w, sem_base, sem_keep, fsend, frecv, bsend, brecv, sem_out, sem_nrm, sem_gp,
):
    s = lax.axis_index("section")
    sections = lax.axis_size("section")
    last = sections - 1
    chunks, rows, width = fin_v.shape
    tokens = base_v.shape[1]
    per_batch = tokens // rows
    block = width // PIECES
    has_next = s < last
    has_prev = s > 0
    nxt = {"section": jnp.minimum(s + 1, last)}
    prv = {"section": jnp.maximum(s - 1, 0)}

    pltpu.make_async_copy(w_hbm.at[0], w_v, sem_w).start()

    @pl.when(s == 0)
    def _():
        pltpu.make_async_copy(inputs_hbm, base_v, sem_base).start()

    @pl.when(has_prev)
    def _():
        pltpu.make_async_copy(stored_hbm.at[0, 0], base_v, sem_base).start()

    pltpu.make_async_copy(stored_hbm.at[0, 1], keep_v, sem_keep).start()

    barrier = pltpu.get_barrier_semaphore()

    @pl.when(has_next)
    def _():
        pl.semaphore_signal(barrier, inc=1, device_id=nxt, device_id_type=MESH)

    @pl.when(has_prev)
    def _():
        pl.semaphore_signal(barrier, inc=1, device_id=prv, device_id_type=MESH)

    pl.semaphore_wait(barrier, jnp.minimum(s, 1) + jnp.minimum(last - s, 1))

    @pl.when(s == 0)
    def _():
        fin_v[...] = jnp.zeros_like(fin_v)

    @pl.when(s == last)
    def _():
        bin_v[...] = jnp.zeros_like(bin_v)

    pltpu.make_async_copy(inputs_hbm, base_v, sem_base).wait()
    pltpu.make_async_copy(stored_hbm.at[0, 1], keep_v, sem_keep).wait()
    pltpu.make_async_copy(w_hbm.at[0], w_v, sem_w).wait()

    def cols_of(j):
        return pl.ds(pl.multiple_of(j * block, block), block)

    def fcopy(c, cols):
        return pltpu.make_async_remote_copy(
            src_ref=clip_v.at[c, :, cols], dst_ref=fin_v.at[c, :, cols],
            send_sem=fsend.at[c], recv_sem=frecv.at[c], device_id=nxt, device_id_type=MESH)

    def fwhole(c):
        return pltpu.make_async_remote_copy(
            src_ref=clip_v.at[c], dst_ref=fin_v.at[c],
            send_sem=fsend.at[c], recv_sem=frecv.at[c], device_id=nxt, device_id_type=MESH)

    def bcopy(c, j):
        cols = cols_of(j)
        return pltpu.make_async_remote_copy(
            src_ref=bout_v.at[c, :, cols], dst_ref=bin_v.at[c, :, cols],
            send_sem=bsend.at[c, j], recv_sem=brecv.at[c, j], device_id=prv, device_id_type=MESH)

    def place(c):
        batch = c // per_batch
        first = pl.multiple_of((c % per_batch) * rows, rows)
        sample = ids_ref[0, batch]
        index = jnp.where(s == 0, batch, sample)
        return batch, first, sample, index

    def forward(c, carry):
        batch, first, sample, index = place(c)

        @pl.when(has_prev)
        def _():
            fwhole(c).wait_recv()

        x = base_v[index, pl.ds(first, rows), :].astype(f32) + fin_v[c].astype(f32)
        mu = jnp.mean(x, axis=-1, keepdims=True)
        xc = x - mu
        var = jnp.mean(xc * xc, axis=-1, keepdims=True)
        rs = lax.rsqrt(var + epsilon)
        normed_v[c] = (xc * rs * gain_ref[...]).astype(bf16)
        mu_v[c] = jnp.broadcast_to(mu, (rows, 128))
        rs_v[c] = jnp.broadcast_to(rs, (rows, 128))

        def tile(j, carry2):
            cols = cols_of(j)
            v = jnp.dot(normed_v[c], w_v[:, cols], preferred_element_type=f32)
            pre_v[c, :, cols] = v
            state = base_v[index, pl.ds(first, rows), cols].astype(f32) + fin_v[c, :, cols].astype(f32)
            res = state + v * (0.5 + 0.5 * lax.erf(v * rsqrt2))
            out_v[c, :, cols] = res.astype(bf16)
            kept = keep_v[sample, pl.ds(first, rows), cols].astype(f32)
            clip_v[c, :, cols] = jnp.clip(res - kept, -delta_bound, delta_bound).astype(bf16)

            @pl.when(has_next)
            def _():
                fcopy(c, cols).start()

            return carry2

        lax.fori_loop(0, PIECES, tile, 0)
        pltpu.make_async_copy(out_v.at[c], out_hbm.at[batch, pl.ds(first, rows)], sem_out.at[c]).start()
        pltpu.make_async_copy(normed_v.at[c], normed_hbm.at[batch, pl.ds(first, rows)], sem_nrm.at[c]).start()
        return carry

    lax.fori_loop(0, chunks, forward, 0)

    def backward(c, carry):
        batch, first, sample, index = place(c)
        acc_v[...] = jnp.zeros_like(acc_v)

        def tile(j, carry2):
            cols = cols_of(j)

            @pl.when(has_next)
            def _():
                bcopy(c, j).wait_recv()

            v = pre_v[c, :, cols]
            cdf = 0.5 + 0.5 * lax.erf(v * rsqrt2)
            slope = cdf + v * (jnp.exp(-0.5 * v * v) * rsqrt2pi)
            state = base_v[index, pl.ds(first, rows), cols].astype(f32) + fin_v[c, :, cols].astype(f32)
            up = jnp.where(s == last, (state + v * cdf) * scale, bin_v[c, :, cols].astype(f32))
            up_v[:, cols] = up
            gp_v[c, :, cols] = (slope * up).astype(bf16)
            acc_v[...] += lax.dot_general(
                gp_v[c, :, cols], w_v[:, cols], (((1,), (1,)), ((), ())), preferred_element_type=f32)
            return carry2

        lax.fori_loop(0, PIECES, tile, 0)
        pltpu.make_async_copy(gp_v.at[c], grad_hbm.at[batch, pl.ds(first, rows)], sem_gp.at[c]).start()
        mu = mu_v[c][:, :1]
        rs = rs_v[c][:, :1]
        x = base_v[index, pl.ds(first, rows), :].astype(f32) + fin_v[c].astype(f32)
        xhat = (x - mu) * rs
        dx = acc_v[...] * gain_ref[...]
        m1 = jnp.mean(dx, axis=-1, keepdims=True)
        m2 = jnp.mean(dx * xhat, axis=-1, keepdims=True)
        bout_v[c] = (up_v[...] + rs * (dx - m1 - xhat * m2)).astype(bf16)

        @pl.when(has_prev)
        def _():
            for j in range(PIECES):
                bcopy(c, j).start()

        return carry

    lax.fori_loop(0, chunks, backward, 0)

    def finish(c, carry):
        batch, first, sample, index = place(c)
        pltpu.make_async_copy(out_v.at[c], out_hbm.at[batch, pl.ds(first, rows)], sem_out.at[c]).wait()
        pltpu.make_async_copy(normed_v.at[c], normed_hbm.at[batch, pl.ds(first, rows)], sem_nrm.at[c]).wait()
        pltpu.make_async_copy(gp_v.at[c], grad_hbm.at[batch, pl.ds(first, rows)], sem_gp.at[c]).wait()

        @pl.when(has_next)
        def _():
            fwhole(c).wait_send()

        @pl.when(has_prev)
        def _():
            for j in range(PIECES):
                bcopy(c, j).wait_send()

        return carry

    lax.fori_loop(0, chunks, finish, 0)


def relay(scale, inputs, sample_ids, stored, weight, norm_gain):
    batches, tokens, width = inputs.shape
    rows = min(CHUNK, tokens)
    chunks = batches * tokens // rows
    shape = jax.ShapeDtypeStruct(inputs.shape, bf16)
    any_spec = pl.BlockSpec(memory_space=pl.ANY)
    chunked = pltpu.VMEM((chunks, rows, width), bf16)
    dma = pltpu.SemaphoreType.DMA
    return pl.pallas_call(
        functools.partial(relay_kernel, scale),
        out_shape=(shape, shape, shape),
        in_specs=[
            pl.BlockSpec(memory_space=pltpu.SMEM), any_spec, any_spec, any_spec,
            pl.BlockSpec(memory_space=pltpu.VMEM),
        ],
        out_specs=(any_spec, any_spec, any_spec),
        scratch_shapes=[
            pltpu.VMEM((width, width), bf16),
            pltpu.VMEM(inputs.shape, bf16),
            pltpu.VMEM(inputs.shape, bf16),
            chunked, chunked, chunked,
            pltpu.VMEM((chunks, rows, width), f32),
            chunked, chunked, chunked, chunked,
            pltpu.VMEM((rows, width), f32),
            pltpu.VMEM((rows, width), f32),
            pltpu.VMEM((chunks, rows, 128), f32),
            pltpu.VMEM((chunks, rows, 128), f32),
            dma, dma, dma,
            dma((chunks,)), dma((chunks,)),
            dma((chunks, PIECES)), dma((chunks, PIECES)),
            dma((chunks,)), dma((chunks,)), dma((chunks,)),
        ],
        compiler_params=pltpu.CompilerParams(
            collective_id=0, has_side_effects=True, vmem_limit_bytes=60 * 1024 * 1024),
        cost_estimate=pl.CostEstimate(
            flops=4 * batches * tokens * width * width, bytes_accessed=2 * width * width, transcendentals=0),
        name="relay",
    )(sample_ids, inputs, stored, weight, norm_gain)


def per_device(inputs, sample_ids, stored, weight, norm_gain):
    batches, tokens, width = inputs.shape
    rows_total = batches * tokens
    scale = 1.0 / math.sqrt(lax.axis_size("dp") * rows_total)
    outs, normed, grads = relay(scale, inputs, sample_ids, stored, weight, norm_gain)
    summed = lax.psum_scatter(
        lax.dot_general(
            normed.reshape(rows_total, width), grads.reshape(rows_total, width),
            (((0,), (0,)), ((), ())), preferred_element_type=f32,
        ).astype(bf16),
        "dp", scatter_dimension=0, tiled=True,
    )
    return (outs[None], summed[None])


def solution(mesh):
    return jax.shard_map(
        per_device,
        mesh=mesh,
        in_specs=(
            P("dp", None, None),
            P("dp", None),
            P("section", None, "dp", None, None),
            P("section", None, None),
            P("section", None),
        ),
        out_specs=(P("section", "dp", None, None), P("section", "dp", None)),
        check_vma=False,
    )
```

```python
import functools
import math

import jax
import jax.numpy as jnp
from jax import lax
from jax.experimental import pallas as pl
from jax.experimental.pallas import tpu as pltpu
from jax.sharding import PartitionSpec as P

epsilon = 1e-05
delta_bound = 2.0
CHUNK = 32
PIECES = 4
GRAD_PIECES = 6
MESH = pl.DeviceIdType.MESH
f32 = jnp.float32
bf16 = jnp.bfloat16
rsqrt2 = 1.0 / math.sqrt(2.0)
rsqrt2pi = 1.0 / math.sqrt(2.0 * math.pi)


def relay_kernel(
    scale,
    ids_ref, inputs_hbm, stored_hbm, w_hbm, gain_ref,
    out_hbm, wgrad_hbm,
    w_v, base_v, keep_v, fin_v, clip_v, normed_v, pre_v, out_v, bin_v, bout_v,
    acc_v, up_v, mu_v, rs_v,
    nt_v, ngat_v, ggat_v, tile_v, csend_v, crecv_v, own_v, ysend_v, yrecv_v, res_v,
    sem_w, sem_base, sem_keep, fsend, frecv, bsend, brecv, sem_out,
    nsend, nrecv, zsend, zrecv, csend, crecv, ysend, yrecv, sem_res,
):
    s = lax.axis_index("section")
    sections = lax.axis_size("section")
    d = lax.axis_index("dp")
    last = sections - 1
    chunks, rows, width = fin_v.shape
    tokens = base_v.shape[1]
    batches = base_v.shape[0]
    local = chunks * rows
    per_batch = tokens // rows
    block = width // PIECES
    has_next = s < last
    has_prev = s > 0
    nxt = {"section": jnp.minimum(s + 1, last)}
    prv = {"section": jnp.maximum(s - 1, 0)}
    z = d // 4
    rest = d % 4
    core = d % 2
    row = rest // 2
    z_up = (z + 1) % 4
    z_down = (z + 3) % 4
    z_far = (z + 2) % 4
    dev_up = {"dp": z_up * 4 + rest}
    dev_down = {"dp": z_down * 4 + rest}
    dev_far = {"dp": z_far * 4 + rest}
    dev_core = {"dp": d + 1 - 2 * core}
    dev_row = {"dp": z * 4 + (rest + 2) % 4}

    pltpu.make_async_copy(w_hbm.at[0], w_v, sem_w).start()

    @pl.when(s == 0)
    def _():
        pltpu.make_async_copy(inputs_hbm, base_v, sem_base).start()

    @pl.when(has_prev)
    def _():
        pltpu.make_async_copy(stored_hbm.at[0, 0], base_v, sem_base).start()

    pltpu.make_async_copy(stored_hbm.at[0, 1], keep_v, sem_keep).start()

    barrier = pltpu.get_barrier_semaphore()

    @pl.when(has_next)
    def _():
        pl.semaphore_signal(barrier, inc=1, device_id=nxt, device_id_type=MESH)

    @pl.when(has_prev)
    def _():
        pl.semaphore_signal(barrier, inc=1, device_id=prv, device_id_type=MESH)

    for peer in (dev_up, dev_down, dev_far, dev_core, dev_row):
        pl.semaphore_signal(barrier, inc=1, device_id=peer, device_id_type=MESH)
    pl.semaphore_wait(barrier, 5 + jnp.minimum(s, 1) + jnp.minimum(last - s, 1))

    @pl.when(s == 0)
    def _():
        fin_v[...] = jnp.zeros_like(fin_v)

    @pl.when(s == last)
    def _():
        bin_v[...] = jnp.zeros_like(bin_v)

    pltpu.make_async_copy(inputs_hbm, base_v, sem_base).wait()
    pltpu.make_async_copy(stored_hbm.at[0, 1], keep_v, sem_keep).wait()
    pltpu.make_async_copy(w_hbm.at[0], w_v, sem_w).wait()

    def remote(src, dst, send, recv, device):
        return pltpu.make_async_remote_copy(
            src_ref=src, dst_ref=dst, send_sem=send, recv_sem=recv, device_id=device, device_id_type=MESH)

    def cols_of(j):
        return pl.ds(pl.multiple_of(j * block, block), block)

    def fcopy(c, cols):
        return remote(clip_v.at[c, :, cols], fin_v.at[c, :, cols], fsend.at[c], frecv.at[c], nxt)

    def fwhole(c):
        return remote(clip_v.at[c], fin_v.at[c], fsend.at[c], frecv.at[c], nxt)

    def bcopy(c, j):
        cols = cols_of(j)
        return remote(bout_v.at[c, :, cols], bin_v.at[c, :, cols], bsend.at[c, j], brecv.at[c, j], prv)

    def place(c):
        batch = c // per_batch
        first = pl.multiple_of((c % per_batch) * rows, rows)
        sample = ids_ref[0, batch]
        index = jnp.where(s == 0, batch, sample)
        return batch, first, sample, index

    share = width // 4
    half = width // 2

    def slot_rows(slot, c):
        return pl.ds(pl.multiple_of(slot * local + c * rows, rows), rows)

    def to_up(c):
        return remote(ggat_v.at[slot_rows(0, c)], ggat_v.at[slot_rows(1, c)], zsend.at[0, c], zrecv.at[0, c], dev_up)

    def to_down(c):
        return remote(ggat_v.at[slot_rows(0, c)], ggat_v.at[slot_rows(2, c)], zsend.at[1, c], zrecv.at[1, c], dev_down)

    def pass_up(c):
        lanes = pl.ds(0, half)
        return remote(ggat_v.at[slot_rows(1, c), lanes], ggat_v.at[slot_rows(3, c), lanes],
                      zsend.at[2, c], zrecv.at[2, c], dev_up)

    def pass_down(c):
        lanes = pl.ds(half, half)
        return remote(ggat_v.at[slot_rows(2, c), lanes], ggat_v.at[slot_rows(3, c), lanes],
                      zsend.at[3, c], zrecv.at[3, c], dev_down)

    def pass_on(c):
        to_up(c).wait_recv()
        pass_up(c).start()
        to_down(c).wait_recv()
        pass_down(c).start()

    def ncopy(slot, z_to, device):
        return remote(nt_v.at[pl.ds(pl.multiple_of(z_to * share, share), share)],
                      ngat_v.at[:, pl.ds(slot * local, local)], nsend.at[slot - 1], nrecv.at[slot - 1], device)

    def share_normed():
        step = 256
        def turn(i, carry):
            cols = pl.ds(pl.multiple_of(i * step, step), step)
            for b in range(batches):
                values = normed_v[pl.ds(b * per_batch, per_batch), :, cols].reshape(tokens, step)
                nt_v[cols, pl.ds(b * tokens, tokens)] = values.T
            return carry
        lax.fori_loop(0, width // step, turn, 0)
        ncopy(1, z_up, dev_up).start()
        ncopy(2, z_down, dev_down).start()
        ncopy(3, z_far, dev_far).start()
        ngat_v[:, pl.ds(0, local)] = nt_v[pl.ds(pl.multiple_of(z * share, share), share)]

    def forward(c, carry):
        batch, first, sample, index = place(c)

        @pl.when(has_prev)
        def _():
            fwhole(c).wait_recv()

        x = base_v[index, pl.ds(first, rows), :].astype(f32) + fin_v[c].astype(f32)
        mu = jnp.mean(x, axis=-1, keepdims=True)
        xc = x - mu
        var = jnp.mean(xc * xc, axis=-1, keepdims=True)
        rs = lax.rsqrt(var + epsilon)
        normed_v[c] = (xc * rs * gain_ref[...]).astype(bf16)
        mu_v[c] = jnp.broadcast_to(mu, (rows, 128))
        rs_v[c] = jnp.broadcast_to(rs, (rows, 128))

        def tile(j, carry2):
            cols = cols_of(j)
            v = jnp.dot(normed_v[c], w_v[:, cols], preferred_element_type=f32)
            pre_v[c, :, cols] = v
            state = base_v[index, pl.ds(first, rows), cols].astype(f32) + fin_v[c, :, cols].astype(f32)
            res = state + v * (0.5 + 0.5 * lax.erf(v * rsqrt2))
            out_v[c, :, cols] = res.astype(bf16)
            kept = keep_v[sample, pl.ds(first, rows), cols].astype(f32)
            clip_v[c, :, cols] = jnp.clip(res - kept, -delta_bound, delta_bound).astype(bf16)

            @pl.when(has_next)
            def _():
                fcopy(c, cols).start()

            return carry2

        lax.fori_loop(0, PIECES, tile, 0)
        pltpu.make_async_copy(out_v.at[c], out_hbm.at[batch, pl.ds(first, rows)], sem_out.at[c]).start()
        return carry

    lax.fori_loop(0, chunks, forward, 0)

    @pl.when(has_next)
    def _():
        share_normed()

    def backward(c, carry):
        batch, first, sample, index = place(c)
        acc_v[...] = jnp.zeros_like(acc_v)

        def tile(j, carry2):
            cols = cols_of(j)

            @pl.when(has_next)
            def _():
                bcopy(c, j).wait_recv()

            v = pre_v[c, :, cols]
            cdf = 0.5 + 0.5 * lax.erf(v * rsqrt2)
            slope = cdf + v * (jnp.exp(-0.5 * v * v) * rsqrt2pi)
            state = base_v[index, pl.ds(first, rows), cols].astype(f32) + fin_v[c, :, cols].astype(f32)
            up = jnp.where(s == last, (state + v * cdf) * scale, bin_v[c, :, cols].astype(f32))
            up_v[:, cols] = up
            gp = (slope * up).astype(bf16)
            ggat_v[slot_rows(0, c), cols] = gp

            @pl.when(has_prev)
            def _():
                acc_v[...] += lax.dot_general(
                    gp, w_v[:, cols], (((1,), (1,)), ((), ())), preferred_element_type=f32)

            return carry2

        lax.fori_loop(0, PIECES, tile, 0)
        to_up(c).start()
        to_down(c).start()

        @pl.when(has_prev)
        def _():
            mu = mu_v[c][:, :1]
            rs = rs_v[c][:, :1]
            x = base_v[index, pl.ds(first, rows), :].astype(f32) + fin_v[c].astype(f32)
            xhat = (x - mu) * rs
            dx = acc_v[...] * gain_ref[...]
            m1 = jnp.mean(dx, axis=-1, keepdims=True)
            m2 = jnp.mean(dx * xhat, axis=-1, keepdims=True)
            bout_v[c] = (up_v[...] + rs * (dx - m1 - xhat * m2)).astype(bf16)
            for j in range(PIECES):
                bcopy(c, j).start()

        @pl.when(c >= 1)
        def _():
            pass_on(c - 1)

        return carry

    lax.fori_loop(0, chunks, backward, 0)
    pass_on(chunks - 1)

    @pl.when(s == last)
    def _():
        share_normed()

    def arrived(c, carry):
        pass_up(c).wait_recv()
        pass_down(c).wait_recv()
        return carry

    ncopy(1, z_up, dev_up).wait_recv()
    ncopy(2, z_down, dev_down).wait_recv()
    ncopy(3, z_far, dev_far).wait_recv()
    lax.fori_loop(0, chunks, arrived, 0)

    part = share // 4
    wide = width // GRAD_PIECES

    def lanes_of(q):
        return pl.ds(pl.multiple_of(q * wide, wide), wide)

    def core_copy(q):
        lanes = lanes_of(q)
        return remote(csend_v.at[:, :, lanes], crecv_v.at[:, :, lanes], csend.at[q], crecv.at[q], dev_core)

    def row_copy(q):
        lanes = lanes_of(q)
        return remote(ysend_v.at[:, lanes], yrecv_v.at[:, lanes], ysend.at[q], yrecv.at[q], dev_row)

    def res_copy(q):
        lanes = lanes_of(q)
        return pltpu.make_async_copy(res_v.at[:, lanes], wgrad_hbm.at[:, lanes], sem_res.at[q])

    def product(q, carry):
        @pl.when(q < GRAD_PIECES)
        def _():
            lanes = lanes_of(q)
            tile_v[...] = jnp.dot(ngat_v[...], ggat_v[:, lanes], preferred_element_type=f32)
            for y in range(2):
                mine = pl.ds(pl.multiple_of(y * 2 * part + core * part, part), part)
                other = pl.ds(pl.multiple_of(y * 2 * part + (1 - core) * part, part), part)
                csend_v[y, :, lanes] = tile_v[other, :].astype(bf16)
                own_v[y, :, lanes] = tile_v[mine, :]
            core_copy(q).start()

        @pl.when(q >= 1)
        def _():
            lanes = lanes_of(q - 1)
            core_copy(q - 1).wait_recv()
            ysend_v[:, lanes] = (own_v[1 - row, :, lanes] + crecv_v[1 - row, :, lanes].astype(f32)).astype(bf16)
            row_copy(q - 1).start()

        return carry

    lax.fori_loop(0, GRAD_PIECES + 1, product, 0)

    def total(q, carry):
        lanes = lanes_of(q)
        row_copy(q).wait_recv()
        res_v[:, lanes] = (
            own_v[row, :, lanes] + crecv_v[row, :, lanes].astype(f32) + yrecv_v[:, lanes].astype(f32)
        ).astype(bf16)
        res_copy(q).start()
        return carry

    lax.fori_loop(0, GRAD_PIECES, total, 0)

    def finish(c, carry):
        batch, first, sample, index = place(c)
        pltpu.make_async_copy(out_v.at[c], out_hbm.at[batch, pl.ds(first, rows)], sem_out.at[c]).wait()
        to_up(c).wait_send()
        to_down(c).wait_send()
        pass_up(c).wait_send()
        pass_down(c).wait_send()

        @pl.when(has_next)
        def _():
            fwhole(c).wait_send()

        @pl.when(has_prev)
        def _():
            for j in range(PIECES):
                bcopy(c, j).wait_send()

        return carry

    lax.fori_loop(0, chunks, finish, 0)

    def finish_grad(q, carry):
        core_copy(q).wait_send()
        row_copy(q).wait_send()
        res_copy(q).wait()
        return carry

    lax.fori_loop(0, GRAD_PIECES, finish_grad, 0)
    ncopy(1, z_up, dev_up).wait_send()
    ncopy(2, z_down, dev_down).wait_send()
    ncopy(3, z_far, dev_far).wait_send()


def relay(scale, inputs, sample_ids, stored, weight, norm_gain):
    batches, tokens, width = inputs.shape
    rows = min(CHUNK, tokens)
    local = batches * tokens
    chunks = local // rows
    share = width // 4
    part = share // 4
    any_spec = pl.BlockSpec(memory_space=pl.ANY)
    chunked = pltpu.VMEM((chunks, rows, width), bf16)
    dma = pltpu.SemaphoreType.DMA
    return pl.pallas_call(
        functools.partial(relay_kernel, scale),
        out_shape=(
            jax.ShapeDtypeStruct(inputs.shape, bf16),
            jax.ShapeDtypeStruct((part, width), bf16),
        ),
        in_specs=[
            pl.BlockSpec(memory_space=pltpu.SMEM), any_spec, any_spec, any_spec,
            pl.BlockSpec(memory_space=pltpu.VMEM),
        ],
        out_specs=(any_spec, any_spec),
        scratch_shapes=[
            pltpu.VMEM((width, width), bf16),
            pltpu.VMEM(inputs.shape, bf16),
            pltpu.VMEM(inputs.shape, bf16),
            chunked, chunked, chunked,
            pltpu.VMEM((chunks, rows, width), f32),
            chunked, chunked, chunked,
            pltpu.VMEM((rows, width), f32),
            pltpu.VMEM((rows, width), f32),
            pltpu.VMEM((chunks, rows, 128), f32),
            pltpu.VMEM((chunks, rows, 128), f32),
            pltpu.VMEM((width, local), bf16),
            pltpu.VMEM((share, 4 * local), bf16),
            pltpu.VMEM((4 * local, width), bf16),
            pltpu.VMEM((share, width // GRAD_PIECES), f32),
            pltpu.VMEM((2, part, width), bf16),
            pltpu.VMEM((2, part, width), bf16),
            pltpu.VMEM((2, part, width), f32),
            pltpu.VMEM((part, width), bf16),
            pltpu.VMEM((part, width), bf16),
            pltpu.VMEM((part, width), bf16),
            dma, dma, dma,
            dma((chunks,)), dma((chunks,)),
            dma((chunks, PIECES)), dma((chunks, PIECES)),
            dma((chunks,)),
            dma((3,)), dma((3,)),
            dma((4, chunks)), dma((4, chunks)),
            dma((GRAD_PIECES,)), dma((GRAD_PIECES,)),
            dma((GRAD_PIECES,)), dma((GRAD_PIECES,)),
            dma((GRAD_PIECES,)),
        ],
        compiler_params=pltpu.CompilerParams(
            collective_id=0, has_side_effects=True, vmem_limit_bytes=67043328),
        cost_estimate=pl.CostEstimate(
            flops=6 * local * width * width, bytes_accessed=2 * width * width, transcendentals=0),
        name="relay",
    )(sample_ids, inputs, stored, weight, norm_gain)


def per_device(inputs, sample_ids, stored, weight, norm_gain):
    batches, tokens, width = inputs.shape
    scale = 1.0 / math.sqrt(lax.axis_size("dp") * batches * tokens)
    outs, summed = relay(scale, inputs, sample_ids, stored, weight, norm_gain)
    return (outs[None], summed[None])


def solution(mesh):
    return jax.shard_map(
        per_device,
        mesh=mesh,
        in_specs=(
            P("dp", None, None),
            P("dp", None),
            P("section", None, "dp", None, None),
            P("section", None, None),
            P("section", None),
        ),
        out_specs=(P("section", "dp", None, None), P("section", "dp", None)),
        check_vma=False,
    )
```

```python
import functools
import math

import jax
import jax.numpy as jnp
from jax import lax
from jax.experimental import pallas as pl
from jax.experimental.pallas import tpu as pltpu
from jax.sharding import PartitionSpec as P

epsilon = 1e-05
delta_bound = 2.0
CHUNK = 32
PIECES = 4
GRAD_PIECES = 6
MESH = pl.DeviceIdType.MESH
f32 = jnp.float32
bf16 = jnp.bfloat16
rsqrt2 = 1.0 / math.sqrt(2.0)
rsqrt2pi = 1.0 / math.sqrt(2.0 * math.pi)


def relay_kernel(
    scale,
    ids_ref, inputs_hbm, stored_hbm, w_hbm, gain_ref,
    out_hbm, wgrad_hbm,
    w_v, wt_v, base_v, keep_v, fin_v, clip_v, normed_v, pre_v, out_v, bin_v,
    up_v, mu_v, rs_v, u_v,
    nt_v, ngat_v, ggat_v, crecv_v, yrecv_v,
    sem_w, sem_base, sem_keep, fsend, frecv, bsend, brecv, sem_out,
    nsend, nrecv, zsend, zrecv, csend, crecv, ysend, yrecv, sem_res,
):
    s = lax.axis_index("section")
    sections = lax.axis_size("section")
    d = lax.axis_index("dp")
    last = sections - 1
    chunks, rows, width = fin_v.shape
    tokens = base_v.shape[1]
    batches = base_v.shape[0]
    local = chunks * rows
    per_batch = tokens // rows
    block = width // PIECES
    has_next = s < last
    has_prev = s > 0
    nxt = {"section": jnp.minimum(s + 1, last)}
    prv = {"section": jnp.maximum(s - 1, 0)}
    z = d // 4
    rest = d % 4
    core = d % 2
    row = rest // 2
    z_up = (z + 1) % 4
    z_down = (z + 3) % 4
    z_far = (z + 2) % 4
    dev_up = {"dp": z_up * 4 + rest}
    dev_down = {"dp": z_down * 4 + rest}
    dev_far = {"dp": z_far * 4 + rest}
    dev_core = {"dp": d + 1 - 2 * core}
    dev_row = {"dp": z * 4 + (rest + 2) % 4}

    pltpu.make_async_copy(w_hbm.at[0], w_v, sem_w).start()

    @pl.when(s == 0)
    def _():
        pltpu.make_async_copy(inputs_hbm, base_v, sem_base).start()

    @pl.when(has_prev)
    def _():
        pltpu.make_async_copy(stored_hbm.at[0, 0], base_v, sem_base).start()

    pltpu.make_async_copy(stored_hbm.at[0, 1], keep_v, sem_keep).start()

    barrier = pltpu.get_barrier_semaphore()

    @pl.when(has_next)
    def _():
        pl.semaphore_signal(barrier, inc=1, device_id=nxt, device_id_type=MESH)

    @pl.when(has_prev)
    def _():
        pl.semaphore_signal(barrier, inc=1, device_id=prv, device_id_type=MESH)

    for peer in (dev_up, dev_down, dev_far, dev_core, dev_row):
        pl.semaphore_signal(barrier, inc=1, device_id=peer, device_id_type=MESH)
    pl.semaphore_wait(barrier, 5 + jnp.minimum(s, 1) + jnp.minimum(last - s, 1))

    @pl.when(s == 0)
    def _():
        fin_v[...] = jnp.zeros_like(fin_v)

    @pl.when(s == last)
    def _():
        bin_v[...] = jnp.zeros_like(bin_v)

    pltpu.make_async_copy(inputs_hbm, base_v, sem_base).wait()
    pltpu.make_async_copy(stored_hbm.at[0, 1], keep_v, sem_keep).wait()
    pltpu.make_async_copy(w_hbm.at[0], w_v, sem_w).wait()

    @pl.when(has_prev)
    def _():
        side = 256
        line = lax.broadcasted_iota(jnp.int32, (side, side), 0)
        column = lax.broadcasted_iota(jnp.int32, (side, side), 1)
        eye = jnp.where(line == column, 1.0, 0.0).astype(bf16)

        def turn(i, carry):
            cols = pl.ds(pl.multiple_of(i * side, side), side)
            for j in range(PIECES):
                part = pl.ds(j * block, block)
                wt_v[cols, part] = lax.dot_general(
                    eye, w_v[part, cols], (((1,), (1,)), ((), ())), preferred_element_type=f32).astype(bf16)
            return carry

        lax.fori_loop(0, width // side, turn, 0)
        high = gain_ref[...].astype(bf16)
        low = (gain_ref[...] - high.astype(f32)).astype(bf16)
        which = lax.broadcasted_iota(jnp.int32, (16, width), 0)
        pair = jnp.where(which == 0, high.astype(f32), jnp.where(which == 1, low.astype(f32), 0.0)).astype(bf16)

        def weigh(j, carry):
            cols = pl.ds(pl.multiple_of(j * block, block), block)
            both = jnp.dot(pair, w_v[:, cols], preferred_element_type=f32)
            u_v[:, cols] = jnp.broadcast_to(jnp.sum(both, axis=0, keepdims=True), (8, block))
            return carry

        lax.fori_loop(0, PIECES, weigh, 0)

    @pl.when(s == 0)
    def _():
        u_v[...] = jnp.zeros_like(u_v)

    def remote(src, dst, send, recv, device):
        return pltpu.make_async_remote_copy(
            src_ref=src, dst_ref=dst, send_sem=send, recv_sem=recv, device_id=device, device_id_type=MESH)

    def cols_of(j):
        return pl.ds(pl.multiple_of(j * block, block), block)

    def fcopy(c, cols):
        return remote(clip_v.at[c, :, cols], fin_v.at[c, :, cols], fsend.at[c], frecv.at[c], nxt)

    def fwhole(c):
        return remote(clip_v.at[c], fin_v.at[c], fsend.at[c], frecv.at[c], nxt)

    def bcopy(c, j):
        cols = cols_of(j)
        return remote(clip_v.at[c, :, cols], bin_v.at[c, :, cols], bsend.at[c, j], brecv.at[c, j], prv)

    def place(c):
        batch = c // per_batch
        first = pl.multiple_of((c % per_batch) * rows, rows)
        sample = ids_ref[0, batch]
        index = jnp.where(s == 0, batch, sample)
        return batch, first, sample, index

    share = width // 4
    half = width // 2

    def slot_rows(slot, c):
        return pl.ds(pl.multiple_of(slot * local + c * rows, rows), rows)

    def to_up(c):
        return remote(ggat_v.at[slot_rows(0, c)], ggat_v.at[slot_rows(1, c)], zsend.at[0, c], zrecv.at[0, c], dev_up)

    def to_down(c):
        return remote(ggat_v.at[slot_rows(0, c)], ggat_v.at[slot_rows(2, c)], zsend.at[1, c], zrecv.at[1, c], dev_down)

    def pass_up(c):
        lanes = pl.ds(0, half)
        return remote(ggat_v.at[slot_rows(1, c), lanes], ggat_v.at[slot_rows(3, c), lanes],
                      zsend.at[2, c], zrecv.at[2, c], dev_up)

    def pass_down(c):
        lanes = pl.ds(half, half)
        return remote(ggat_v.at[slot_rows(2, c), lanes], ggat_v.at[slot_rows(3, c), lanes],
                      zsend.at[3, c], zrecv.at[3, c], dev_down)

    def pass_on(c):
        to_up(c).wait_recv()
        pass_up(c).start()
        to_down(c).wait_recv()
        pass_down(c).start()

    def ncopy(slot, z_to, device):
        return remote(nt_v.at[pl.ds(pl.multiple_of(z_to * share, share), share)],
                      ngat_v.at[:, pl.ds(slot * local, local)], nsend.at[slot - 1], nrecv.at[slot - 1], device)

    def share_normed():
        step = 256
        def turn(i, carry):
            cols = pl.ds(pl.multiple_of(i * step, step), step)
            for b in range(batches):
                values = normed_v[pl.ds(b * per_batch, per_batch), :, cols].reshape(tokens, step)
                nt_v[cols, pl.ds(b * tokens, tokens)] = values.T
            return carry
        lax.fori_loop(0, width // step, turn, 0)
        ncopy(1, z_up, dev_up).start()
        ncopy(2, z_down, dev_down).start()
        ncopy(3, z_far, dev_far).start()
        ngat_v[:, pl.ds(0, local)] = nt_v[pl.ds(pl.multiple_of(z * share, share), share)]

    def forward(c):
        batch, first, sample, index = place(c)

        @pl.when(has_prev)
        def _():
            fwhole(c).wait_recv()

        x = base_v[index, pl.ds(first, rows), :].astype(f32) + fin_v[c].astype(f32)
        mu = jnp.mean(x, axis=-1, keepdims=True)
        xc = x - mu
        var = jnp.mean(xc * xc, axis=-1, keepdims=True)
        rs = lax.rsqrt(var + epsilon)
        normed_v[c] = (xc * rs * gain_ref[...]).astype(bf16)
        mu_v[c] = jnp.broadcast_to(mu, (rows, 128))
        rs_v[c] = jnp.broadcast_to(rs, (rows, 128))

        def tile(j, carry2):
            cols = cols_of(j)
            v = jnp.dot(normed_v[c], w_v[:, cols], preferred_element_type=f32)
            pre_v[c, :, cols] = v
            state = base_v[index, pl.ds(first, rows), cols].astype(f32) + fin_v[c, :, cols].astype(f32)
            res = state + v * (0.5 + 0.5 * lax.erf(v * rsqrt2))
            out_v[c, :, cols] = res.astype(bf16)
            kept = keep_v[sample, pl.ds(first, rows), cols].astype(f32)
            clip_v[c, :, cols] = jnp.clip(res - kept, -delta_bound, delta_bound).astype(bf16)

            @pl.when(has_next)
            def _():
                fcopy(c, cols).start()

            return carry2

        lax.fori_loop(0, PIECES, tile, 0)
        pltpu.make_async_copy(out_v.at[c], out_hbm.at[batch, pl.ds(first, rows)], sem_out.at[c]).start()

    def backward(c):
        batch, first, sample, index = place(c)

        def piece(j, sums):
            cols = cols_of(j)

            @pl.when(has_next)
            def _():
                bcopy(c, j).wait_recv()

            v = pre_v[c, :, cols]
            cdf = 0.5 + 0.5 * lax.erf(v * rsqrt2)
            slope = cdf + v * (jnp.exp(-0.5 * v * v) * rsqrt2pi)
            state = base_v[index, pl.ds(first, rows), cols].astype(f32) + fin_v[c, :, cols].astype(f32)
            up = jnp.where(s == last, (state + v * cdf) * scale, bin_v[c, :, cols].astype(f32))
            up_v[:, cols] = up
            gp = (slope * up).astype(bf16)
            ggat_v[slot_rows(0, c), cols] = gp
            wide_gp = gp.astype(f32)
            return (
                sums[0] + jnp.sum(wide_gp * u_v[0:1, cols], axis=-1, keepdims=True),
                sums[1] + jnp.sum(wide_gp * v, axis=-1, keepdims=True),
            )

        zero = jnp.zeros((rows, 1), f32)
        sums = lax.fori_loop(0, PIECES, piece, (zero, zero))
        to_up(c).start()
        to_down(c).start()

        @pl.when(has_prev)
        def _():
            m1 = sums[0] * (1.0 / width)
            m2 = sums[1] * (1.0 / width)
            mu = mu_v[c][:, :1]
            rs = rs_v[c][:, :1]

            @pl.when(has_next)
            def _():
                fwhole(c).wait_send()

            def tile(j, carry2):
                cols = cols_of(j)
                gn = jnp.dot(ggat_v[slot_rows(0, c)], wt_v[:, cols], preferred_element_type=f32)
                state = base_v[index, pl.ds(first, rows), cols].astype(f32) + fin_v[c, :, cols].astype(f32)
                xhat = (state - mu) * rs
                clip_v[c, :, cols] = (
                    up_v[:, cols] + rs * (gn * gain_ref[:, cols] - m1 - xhat * m2)
                ).astype(bf16)
                bcopy(c, j).start()
                return carry2

            lax.fori_loop(0, PIECES, tile, 0)

        @pl.when(c >= 1)
        def _():
            pass_on(c - 1)

    ahead = jnp.minimum(chunks, ((last - s) * 7 + 1) // 2)
    early = ahead == chunks

    def step(t, carry):
        @pl.when(t < chunks)
        def _():
            forward(t)

        @pl.when(jnp.logical_and(t == chunks - 1, early))
        def _():
            share_normed()

        @pl.when(t >= ahead)
        def _():
            backward(t - ahead)

        return carry

    lax.fori_loop(0, chunks + ahead, step, 0)
    pass_on(chunks - 1)

    @pl.when(jnp.logical_not(early))
    def _():
        share_normed()

    def arrived(c, carry):
        pass_up(c).wait_recv()
        pass_down(c).wait_recv()
        return carry

    ncopy(1, z_up, dev_up).wait_recv()
    ncopy(2, z_down, dev_down).wait_recv()
    ncopy(3, z_far, dev_far).wait_recv()
    lax.fori_loop(0, chunks, arrived, 0)

    part = share // 4
    wide = width // GRAD_PIECES

    def lanes_of(q):
        return pl.ds(pl.multiple_of(q * wide, wide), wide)

    def held(place_of):
        return pl.ds(place_of * part, part)

    def core_copy(q, y):
        lanes = lanes_of(q)
        return remote(w_v.at[held(y), lanes], crecv_v.at[y, :, lanes], csend.at[q, y], crecv.at[q, y], dev_core)

    def row_copy(q):
        lanes = lanes_of(q)
        return remote(w_v.at[held(4), lanes], yrecv_v.at[:, lanes], ysend.at[q], yrecv.at[q], dev_row)

    def res_copy(q):
        lanes = lanes_of(q)
        return pltpu.make_async_copy(w_v.at[held(5), lanes], wgrad_hbm.at[:, lanes], sem_res.at[q])

    def band(y, whose):
        return pl.ds(pl.multiple_of(y * 2 * part + whose * part, part), part)

    def own_rows(y):
        return pl.ds(pl.multiple_of((2 + y) * part, part), part)

    def product(q, carry):
        @pl.when(q < GRAD_PIECES)
        def _():
            lanes = lanes_of(q)
            for y in range(2):
                w_v[held(y), lanes] = jnp.dot(
                    ngat_v[band(y, 1 - core), :], ggat_v[:, lanes], preferred_element_type=f32).astype(bf16)
                core_copy(q, y).start()
            for y in range(2):
                w_v[held(2 + y), lanes] = jnp.dot(
                    ngat_v[band(y, core), :], ggat_v[:, lanes], preferred_element_type=f32).astype(bf16)

        @pl.when(q >= 1)
        def _():
            lanes = lanes_of(q - 1)
            for y in range(2):
                core_copy(q - 1, y).wait_recv()
            w_v[held(4), lanes] = (
                w_v[own_rows(1 - row), lanes].astype(f32) + crecv_v[1 - row, :, lanes].astype(f32)
            ).astype(bf16)
            row_copy(q - 1).start()

        return carry

    lax.fori_loop(0, GRAD_PIECES + 1, product, 0)

    def total(q, carry):
        lanes = lanes_of(q)
        row_copy(q).wait_recv()
        w_v[held(5), lanes] = (
            w_v[own_rows(row), lanes].astype(f32) + crecv_v[row, :, lanes].astype(f32)
            + yrecv_v[:, lanes].astype(f32)
        ).astype(bf16)
        res_copy(q).start()
        return carry

    lax.fori_loop(0, GRAD_PIECES, total, 0)

    def finish(c, carry):
        batch, first, sample, index = place(c)
        pltpu.make_async_copy(out_v.at[c], out_hbm.at[batch, pl.ds(first, rows)], sem_out.at[c]).wait()
        to_up(c).wait_send()
        to_down(c).wait_send()
        pass_up(c).wait_send()
        pass_down(c).wait_send()

        @pl.when(s == 0)
        def _():
            fwhole(c).wait_send()

        @pl.when(has_prev)
        def _():
            for j in range(PIECES):
                bcopy(c, j).wait_send()

        return carry

    lax.fori_loop(0, chunks, finish, 0)

    def finish_grad(q, carry):
        for y in range(2):
            core_copy(q, y).wait_send()
        row_copy(q).wait_send()
        res_copy(q).wait()
        return carry

    lax.fori_loop(0, GRAD_PIECES, finish_grad, 0)
    ncopy(1, z_up, dev_up).wait_send()
    ncopy(2, z_down, dev_down).wait_send()
    ncopy(3, z_far, dev_far).wait_send()


def relay(scale, inputs, sample_ids, stored, weight, norm_gain):
    batches, tokens, width = inputs.shape
    rows = min(CHUNK, tokens)
    local = batches * tokens
    chunks = local // rows
    share = width // 4
    part = share // 4
    any_spec = pl.BlockSpec(memory_space=pl.ANY)
    chunked = pltpu.VMEM((chunks, rows, width), bf16)
    dma = pltpu.SemaphoreType.DMA
    return pl.pallas_call(
        functools.partial(relay_kernel, scale),
        out_shape=(
            jax.ShapeDtypeStruct(inputs.shape, bf16),
            jax.ShapeDtypeStruct((part, width), bf16),
        ),
        in_specs=[
            pl.BlockSpec(memory_space=pltpu.SMEM), any_spec, any_spec, any_spec,
            pl.BlockSpec(memory_space=pltpu.VMEM),
        ],
        out_specs=(any_spec, any_spec),
        scratch_shapes=[
            pltpu.VMEM((width, width), bf16),
            pltpu.VMEM((width, width), bf16),
            pltpu.VMEM(inputs.shape, bf16),
            pltpu.VMEM(inputs.shape, bf16),
            chunked, chunked, chunked,
            pltpu.VMEM((chunks, rows, width), f32),
            chunked, chunked,
            pltpu.VMEM((rows, width), f32),
            pltpu.VMEM((chunks, rows, 128), f32),
            pltpu.VMEM((chunks, rows, 128), f32),
            pltpu.VMEM((8, width), f32),
            pltpu.VMEM((width, local), bf16),
            pltpu.VMEM((share, 4 * local), bf16),
            pltpu.VMEM((4 * local, width), bf16),
            pltpu.VMEM((2, part, width), bf16),
            pltpu.VMEM((part, width), bf16),
            dma, dma, dma,
            dma((chunks,)), dma((chunks,)),
            dma((chunks, PIECES)), dma((chunks, PIECES)),
            dma((chunks,)),
            dma((3,)), dma((3,)),
            dma((4, chunks)), dma((4, chunks)),
            dma((GRAD_PIECES, 2)), dma((GRAD_PIECES, 2)),
            dma((GRAD_PIECES,)), dma((GRAD_PIECES,)),
            dma((GRAD_PIECES,)),
        ],
        compiler_params=pltpu.CompilerParams(
            collective_id=0, has_side_effects=True, vmem_limit_bytes=67043328),
        cost_estimate=pl.CostEstimate(
            flops=6 * local * width * width, bytes_accessed=2 * width * width, transcendentals=0),
        name="relay",
    )(sample_ids, inputs, stored, weight, norm_gain)


def per_device(inputs, sample_ids, stored, weight, norm_gain):
    batches, tokens, width = inputs.shape
    scale = 1.0 / math.sqrt(lax.axis_size("dp") * batches * tokens)
    outs, summed = relay(scale, inputs, sample_ids, stored, weight, norm_gain)
    return (outs[None], summed[None])


def solution(mesh):
    return jax.shard_map(
        per_device,
        mesh=mesh,
        in_specs=(
            P("dp", None, None),
            P("dp", None),
            P("section", None, "dp", None, None),
            P("section", None, None),
            P("section", None),
        ),
        out_specs=(P("section", "dp", None, None), P("section", "dp", None)),
        check_vma=False,
    )
```

```python
import functools
import math

import jax
import jax.numpy as jnp
from jax import lax
from jax.experimental import pallas as pl
from jax.experimental.pallas import tpu as pltpu
from jax.sharding import PartitionSpec as P

epsilon = 1e-05
delta_bound = 2.0
CHUNK = 32
PIECES = 4
GRAD_PIECES = 6
MESH = pl.DeviceIdType.MESH
f32 = jnp.float32
bf16 = jnp.bfloat16
rsqrt2 = 1.0 / math.sqrt(2.0)
rsqrt2pi = 1.0 / math.sqrt(2.0 * math.pi)


def relay_kernel(
    scale,
    ids_ref, inputs_hbm, stored_hbm, w_hbm, gain_ref,
    out_hbm, wgrad_hbm,
    w_v, wt_v, base_v, keep_v, fin_v, clip_v, normed_v, pre_v, out_v, bin_v,
    mu_v, rs_v, u_v,
    nt_v, ngat_v, ggat_v, crecv_v, yrecv_v,
    sem_w, sem_base, sem_keep, fsend, frecv, bsend, brecv, sem_out,
    nsend, nrecv, zsend, zrecv, csend, crecv, ysend, yrecv, sem_res,
):
    s = lax.axis_index("section")
    sections = lax.axis_size("section")
    d = lax.axis_index("dp")
    last = sections - 1
    chunks, rows, width = fin_v.shape
    tokens = base_v.shape[1]
    batches = base_v.shape[0]
    local = chunks * rows
    per_batch = tokens // rows
    block = width // PIECES
    has_next = s < last
    has_prev = s > 0
    nxt = {"section": jnp.minimum(s + 1, last)}
    prv = {"section": jnp.maximum(s - 1, 0)}
    z = d // 4
    rest = d % 4
    core = d % 2
    row = rest // 2
    z_up = (z + 1) % 4
    z_down = (z + 3) % 4
    z_far = (z + 2) % 4
    dev_up = {"dp": z_up * 4 + rest}
    dev_down = {"dp": z_down * 4 + rest}
    dev_far = {"dp": z_far * 4 + rest}
    dev_core = {"dp": d + 1 - 2 * core}
    dev_row = {"dp": z * 4 + (rest + 2) % 4}

    late = s < last - 2

    def w_copy(j):
        cols = pl.ds(pl.multiple_of(j * block, block), block)
        return pltpu.make_async_copy(w_hbm.at[0, :, cols], w_v.at[:, cols], sem_w.at[j])

    @pl.when(s == 0)
    def _():
        pltpu.make_async_copy(inputs_hbm, base_v, sem_base).start()

    @pl.when(has_prev)
    def _():
        pltpu.make_async_copy(stored_hbm.at[0, 0], base_v, sem_base).start()

    for j in range(PIECES):
        w_copy(j).start()
    pltpu.make_async_copy(stored_hbm.at[0, 1], keep_v, sem_keep).start()

    barrier = pltpu.get_barrier_semaphore()

    @pl.when(has_next)
    def _():
        pl.semaphore_signal(barrier, inc=1, device_id=nxt, device_id_type=MESH)

    @pl.when(has_prev)
    def _():
        pl.semaphore_signal(barrier, inc=1, device_id=prv, device_id_type=MESH)

    for peer in (dev_up, dev_down, dev_far, dev_core, dev_row):
        pl.semaphore_signal(barrier, inc=1, device_id=peer, device_id_type=MESH)
    pl.semaphore_wait(barrier, 5 + jnp.minimum(s, 1) + jnp.minimum(last - s, 1))

    @pl.when(s == 0)
    def _():
        fin_v[...] = jnp.zeros_like(fin_v)

    pltpu.make_async_copy(inputs_hbm, base_v, sem_base).wait()
    def prepare():
        side = 256
        line = lax.broadcasted_iota(jnp.int32, (side, side), 0)
        column = lax.broadcasted_iota(jnp.int32, (side, side), 1)
        eye = jnp.where(line == column, 1.0, 0.0).astype(bf16)

        def turn(i, carry):
            cols = pl.ds(pl.multiple_of(i * side, side), side)
            for j in range(PIECES):
                part = pl.ds(j * block, block)
                wt_v[cols, part] = lax.dot_general(
                    eye, w_v[part, cols], (((1,), (1,)), ((), ())), preferred_element_type=f32).astype(bf16)
            return carry

        lax.fori_loop(0, width // side, turn, 0)
        high = gain_ref[...].astype(bf16)
        low = (gain_ref[...] - high.astype(f32)).astype(bf16)
        which = lax.broadcasted_iota(jnp.int32, (16, width), 0)
        pair = jnp.where(which == 0, high.astype(f32), jnp.where(which == 1, low.astype(f32), 0.0)).astype(bf16)

        def weigh(j, carry):
            cols = pl.ds(pl.multiple_of(j * block, block), block)
            both = jnp.dot(pair, w_v[:, cols], preferred_element_type=f32)
            u_v[:, cols] = jnp.broadcast_to(jnp.sum(both, axis=0, keepdims=True), (8, block))
            return carry

        lax.fori_loop(0, PIECES, weigh, 0)

    @pl.when(s == 0)
    def _():
        u_v[...] = jnp.zeros_like(u_v)

    @pl.when(jnp.logical_not(late))
    def _():
        for j in range(PIECES):
            w_copy(j).wait()
        prepare()

    pltpu.make_async_copy(stored_hbm.at[0, 1], keep_v, sem_keep).wait()

    def remote(src, dst, send, recv, device):
        return pltpu.make_async_remote_copy(
            src_ref=src, dst_ref=dst, send_sem=send, recv_sem=recv, device_id=device, device_id_type=MESH)

    def cols_of(j):
        return pl.ds(pl.multiple_of(j * block, block), block)

    def fcopy(c, cols):
        return remote(clip_v.at[c, :, cols], fin_v.at[c, :, cols], fsend.at[c], frecv.at[c], nxt)

    def fwhole(c):
        return remote(clip_v.at[c], fin_v.at[c], fsend.at[c], frecv.at[c], nxt)

    def bcopy(c, j):
        cols = cols_of(j)
        return remote(clip_v.at[c, :, cols], bin_v.at[c, :, cols], bsend.at[c, j], brecv.at[c, j], prv)

    def place(c):
        batch = c // per_batch
        first = pl.multiple_of((c % per_batch) * rows, rows)
        sample = ids_ref[0, batch]
        index = jnp.where(s == 0, batch, sample)
        return batch, first, sample, index

    share = width // 4
    half = width // 2

    def slot_rows(slot, c, n=1):
        return pl.ds(pl.multiple_of(slot * local + c * rows, rows), n * rows)

    def out_copy(c):
        batch, first, sample, index = place(c)
        return pltpu.make_async_copy(out_v.at[c], out_hbm.at[batch, pl.ds(first, rows)], sem_out.at[c])

    def to_up(c):
        return remote(ggat_v.at[slot_rows(0, c)], ggat_v.at[slot_rows(1, c)], zsend.at[0, c], zrecv.at[0, c], dev_up)

    def to_down(c):
        return remote(ggat_v.at[slot_rows(0, c)], ggat_v.at[slot_rows(2, c)], zsend.at[1, c], zrecv.at[1, c], dev_down)

    def pass_up(c):
        lanes = pl.ds(0, half)
        return remote(ggat_v.at[slot_rows(1, c), lanes], ggat_v.at[slot_rows(3, c), lanes],
                      zsend.at[2, c], zrecv.at[2, c], dev_up)

    def pass_down(c):
        lanes = pl.ds(half, half)
        return remote(ggat_v.at[slot_rows(2, c), lanes], ggat_v.at[slot_rows(3, c), lanes],
                      zsend.at[3, c], zrecv.at[3, c], dev_down)

    def pass_on(c):
        to_up(c).wait_recv()
        pass_up(c).start()
        to_down(c).wait_recv()
        pass_down(c).start()

    def ncopy(slot, z_to, device):
        return remote(nt_v.at[pl.ds(pl.multiple_of(z_to * share, share), share)],
                      ngat_v.at[:, pl.ds(slot * local, local)], nsend.at[slot - 1], nrecv.at[slot - 1], device)

    def share_normed():
        step = 256
        def turn(i, carry):
            cols = pl.ds(pl.multiple_of(i * step, step), step)
            for b in range(batches):
                values = normed_v[pl.ds(b * per_batch, per_batch), :, cols].reshape(tokens, step)
                nt_v[cols, pl.ds(b * tokens, tokens)] = values.T
            return carry
        lax.fori_loop(0, width // step, turn, 0)
        ncopy(1, z_up, dev_up).start()
        ncopy(2, z_down, dev_down).start()
        ncopy(3, z_far, dev_far).start()
        ngat_v[:, pl.ds(0, local)] = nt_v[pl.ds(pl.multiple_of(z * share, share), share)]

    def several(ref, c, n, cols=None):
        if cols is None:
            return ref[pl.ds(c, n)].reshape(n * rows, ref.shape[-1])
        return ref[pl.ds(c, n), :, cols].reshape(n * rows, cols.size)

    def keep(ref, c, n, value, cols=None):
        if cols is None:
            ref[pl.ds(c, n)] = value.reshape(n, rows, value.shape[-1])
        else:
            ref[pl.ds(c, n), :, cols] = value.reshape(n, rows, cols.size)

    def state_of(c, n, cols=None):
        batch, first, sample, index = place(c)
        if cols is None:
            return base_v[index, pl.ds(first, n * rows), :].astype(f32) + several(fin_v, c, n).astype(f32)
        return base_v[index, pl.ds(first, n * rows), cols].astype(f32) + several(fin_v, c, n, cols).astype(f32)

    def forward(c, n, final):
        batch, first, sample, index = place(c)
        if final:
            for i in range(n):
                fwhole(c + i).wait_recv()
        else:
            @pl.when(has_prev)
            def _():
                fwhole(c).wait_recv()

        x = state_of(c, n)
        mu = jnp.mean(x, axis=-1, keepdims=True)
        xc = x - mu
        var = jnp.mean(xc * xc, axis=-1, keepdims=True)
        rs = lax.rsqrt(var + epsilon)
        keep(normed_v, c, n, (xc * rs * gain_ref[...]).astype(bf16))
        keep(mu_v, c, n, jnp.broadcast_to(mu, (n * rows, 128)))
        keep(rs_v, c, n, jnp.broadcast_to(rs, (n * rows, 128)))

        def tile(j, carry2):
            cols = cols_of(j)
            if not final:
                @pl.when(jnp.logical_and(c == 0, late))
                def _():
                    w_copy(j).wait()

            v = jnp.dot(several(normed_v, c, n), w_v[:, cols], preferred_element_type=f32)
            keep(pre_v, c, n, v, cols)
            res = state_of(c, n, cols) + v * (0.5 + 0.5 * lax.erf(v * rsqrt2))
            keep(out_v, c, n, res.astype(bf16), cols)
            if not final:
                kept = keep_v[sample, pl.ds(first, rows), cols].astype(f32)
                clip_v[c, :, cols] = jnp.clip(res - kept, -delta_bound, delta_bound).astype(bf16)
                fcopy(c, cols).start()
            return carry2

        lax.fori_loop(0, PIECES, tile, 0)
        for i in range(n):
            out_copy(c + i).start()

    def backward(c, n, final):
        def piece(j, sums):
            cols = cols_of(j)
            if not final:
                bcopy(c, j).wait_recv()
            v = several(pre_v, c, n, cols)
            cdf = 0.5 + 0.5 * lax.erf(v * rsqrt2)
            slope = cdf + v * (jnp.exp(-0.5 * v * v) * rsqrt2pi)
            if final:
                up = (state_of(c, n, cols) + v * cdf) * scale
            else:
                up = several(bin_v, c, n, cols).astype(f32)
            gp = (slope * up).astype(bf16)
            ggat_v[slot_rows(0, c, n), cols] = gp
            wide_gp = gp.astype(f32)
            return (
                sums[0] + jnp.sum(wide_gp * u_v[0:1, cols], axis=-1, keepdims=True),
                sums[1] + jnp.sum(wide_gp * v, axis=-1, keepdims=True),
            )

        zero = jnp.zeros((n * rows, 1), f32)
        sums = lax.fori_loop(0, PIECES, piece, (zero, zero))
        for i in range(n):
            to_up(c + i).start()
            to_down(c + i).start()

        def pull():
            m1 = sums[0] * (1.0 / width)
            m2 = sums[1] * (1.0 / width)
            mu = several(mu_v, c, n)[:, :1]
            rs = several(rs_v, c, n)[:, :1]
            if not final:
                fwhole(c).wait_send()

            def tile(j, carry2):
                cols = cols_of(j)
                gn = jnp.dot(ggat_v[slot_rows(0, c, n)], wt_v[:, cols], preferred_element_type=f32)
                state = state_of(c, n, cols)
                xhat = (state - mu) * rs
                if final:
                    v = several(pre_v, c, n, cols)
                    up = (state + v * (0.5 + 0.5 * lax.erf(v * rsqrt2))) * scale
                else:
                    up = several(bin_v, c, n, cols).astype(f32)
                sent = up + rs * (gn * gain_ref[:, cols] - m1 - xhat * m2)
                keep(clip_v, c, n, sent.astype(bf16), cols)
                bcopy(c, j).start()
                return carry2

            lax.fori_loop(0, PIECES, tile, 0)
            for i in range(1, n):
                for j in range(PIECES):
                    bcopy(c + i, j).start()

        if final:
            pull()
        else:
            pl.when(has_prev)(pull)

    ahead = jnp.where(s == last - 1, chunks - 2, chunks)

    def step(t, carry):
        @pl.when(t < chunks)
        def _():
            forward(t, 1, False)

        @pl.when(jnp.logical_and(t == chunks - 1, late))
        def _():
            share_normed()

            @pl.when(has_prev)
            def _():
                prepare()

        @pl.when(t > ahead)
        def _():
            pass_on(t - ahead - 1)

        @pl.when(t >= ahead)
        def _():
            backward(t - ahead, 1, False)

        return carry

    def pair_step(t, carry):
        forward(2 * t, 2, True)

        @pl.when(t > 0)
        def _():
            pass_on(2 * t - 2)
            pass_on(2 * t - 1)

        backward(2 * t, 2, True)
        return carry

    @pl.when(has_next)
    def _():
        lax.fori_loop(0, chunks + ahead, step, 0)

    @pl.when(s == last)
    def _():
        lax.fori_loop(0, chunks // 2, pair_step, 0)
        pass_on(chunks - 2)

    pass_on(chunks - 1)

    @pl.when(jnp.logical_not(late))
    def _():
        share_normed()

    def arrived(c, carry):
        pass_up(c).wait_recv()
        pass_down(c).wait_recv()
        return carry

    ncopy(1, z_up, dev_up).wait_recv()
    ncopy(2, z_down, dev_down).wait_recv()
    ncopy(3, z_far, dev_far).wait_recv()
    lax.fori_loop(0, chunks, arrived, 0)

    part = share // 4
    wide = width // GRAD_PIECES

    def lanes_of(q):
        return pl.ds(pl.multiple_of(q * wide, wide), wide)

    def held(place_of):
        return pl.ds(place_of * part, part)

    def core_copy(q, y):
        lanes = lanes_of(q)
        return remote(w_v.at[held(y), lanes], crecv_v.at[y, :, lanes], csend.at[q, y], crecv.at[q, y], dev_core)

    def row_copy(q):
        lanes = lanes_of(q)
        return remote(w_v.at[held(4), lanes], yrecv_v.at[:, lanes], ysend.at[q], yrecv.at[q], dev_row)

    def res_copy(q):
        lanes = lanes_of(q)
        return pltpu.make_async_copy(w_v.at[held(5), lanes], wgrad_hbm.at[:, lanes], sem_res.at[q])

    def band(y, whose):
        return pl.ds(pl.multiple_of(y * 2 * part + whose * part, part), part)

    def own_rows(y):
        return pl.ds(pl.multiple_of((2 + y) * part, part), part)

    def product(q, carry):
        @pl.when(q < GRAD_PIECES)
        def _():
            lanes = lanes_of(q)
            for y in range(2):
                w_v[held(y), lanes] = jnp.dot(
                    ngat_v[band(y, 1 - core), :], ggat_v[:, lanes], preferred_element_type=f32).astype(bf16)
                core_copy(q, y).start()
            for y in range(2):
                w_v[held(2 + y), lanes] = jnp.dot(
                    ngat_v[band(y, core), :], ggat_v[:, lanes], preferred_element_type=f32).astype(bf16)

        @pl.when(q >= 1)
        def _():
            lanes = lanes_of(q - 1)
            for y in range(2):
                core_copy(q - 1, y).wait_recv()
            w_v[held(4), lanes] = (
                w_v[own_rows(1 - row), lanes].astype(f32) + crecv_v[1 - row, :, lanes].astype(f32)
            ).astype(bf16)
            row_copy(q - 1).start()

        return carry

    lax.fori_loop(0, GRAD_PIECES + 1, product, 0)

    def total(q, carry):
        lanes = lanes_of(q)
        row_copy(q).wait_recv()
        w_v[held(5), lanes] = (
            w_v[own_rows(row), lanes].astype(f32) + crecv_v[row, :, lanes].astype(f32)
            + yrecv_v[:, lanes].astype(f32)
        ).astype(bf16)
        res_copy(q).start()
        return carry

    lax.fori_loop(0, GRAD_PIECES, total, 0)

    def finish(c, carry):
        out_copy(c).wait()
        to_up(c).wait_send()
        to_down(c).wait_send()
        pass_up(c).wait_send()
        pass_down(c).wait_send()

        @pl.when(s == 0)
        def _():
            fwhole(c).wait_send()

        @pl.when(has_prev)
        def _():
            for j in range(PIECES):
                bcopy(c, j).wait_send()

        return carry

    lax.fori_loop(0, chunks, finish, 0)

    def finish_grad(q, carry):
        for y in range(2):
            core_copy(q, y).wait_send()
        row_copy(q).wait_send()
        res_copy(q).wait()
        return carry

    lax.fori_loop(0, GRAD_PIECES, finish_grad, 0)
    ncopy(1, z_up, dev_up).wait_send()
    ncopy(2, z_down, dev_down).wait_send()
    ncopy(3, z_far, dev_far).wait_send()


def relay(scale, inputs, sample_ids, stored, weight, norm_gain):
    batches, tokens, width = inputs.shape
    rows = min(CHUNK, tokens)
    local = batches * tokens
    chunks = local // rows
    share = width // 4
    part = share // 4
    any_spec = pl.BlockSpec(memory_space=pl.ANY)
    chunked = pltpu.VMEM((chunks, rows, width), bf16)
    dma = pltpu.SemaphoreType.DMA
    return pl.pallas_call(
        functools.partial(relay_kernel, scale),
        out_shape=(
            jax.ShapeDtypeStruct(inputs.shape, bf16),
            jax.ShapeDtypeStruct((part, width), bf16),
        ),
        in_specs=[
            pl.BlockSpec(memory_space=pltpu.SMEM), any_spec, any_spec, any_spec,
            pl.BlockSpec(memory_space=pltpu.VMEM),
        ],
        out_specs=(any_spec, any_spec),
        scratch_shapes=[
            pltpu.VMEM((width, width), bf16),
            pltpu.VMEM((width, width), bf16),
            pltpu.VMEM(inputs.shape, bf16),
            pltpu.VMEM(inputs.shape, bf16),
            chunked, chunked, chunked,
            pltpu.VMEM((chunks, rows, width), f32),
            chunked, chunked,
            pltpu.VMEM((chunks, rows, 128), f32),
            pltpu.VMEM((chunks, rows, 128), f32),
            pltpu.VMEM((8, width), f32),
            pltpu.VMEM((width, local), bf16),
            pltpu.VMEM((share, 4 * local), bf16),
            pltpu.VMEM((4 * local, width), bf16),
            pltpu.VMEM((2, part, width), bf16),
            pltpu.VMEM((part, width), bf16),
            dma((PIECES,)), dma, dma,
            dma((chunks,)), dma((chunks,)),
            dma((chunks, PIECES)), dma((chunks, PIECES)),
            dma((chunks,)),
            dma((3,)), dma((3,)),
            dma((4, chunks)), dma((4, chunks)),
            dma((GRAD_PIECES, 2)), dma((GRAD_PIECES, 2)),
            dma((GRAD_PIECES,)), dma((GRAD_PIECES,)),
            dma((GRAD_PIECES,)),
        ],
        compiler_params=pltpu.CompilerParams(
            collective_id=0, has_side_effects=True, vmem_limit_bytes=67043328),
        cost_estimate=pl.CostEstimate(
            flops=6 * local * width * width, bytes_accessed=2 * width * width, transcendentals=0),
        name="relay",
    )(sample_ids, inputs, stored, weight, norm_gain)


def per_device(inputs, sample_ids, stored, weight, norm_gain):
    batches, tokens, width = inputs.shape
    scale = 1.0 / math.sqrt(lax.axis_size("dp") * batches * tokens)
    outs, summed = relay(scale, inputs, sample_ids, stored, weight, norm_gain)
    return (outs[None], summed[None])


def solution(mesh):
    return jax.shard_map(
        per_device,
        mesh=mesh,
        in_specs=(
            P("dp", None, None),
            P("dp", None),
            P("section", None, "dp", None, None),
            P("section", None, None),
            P("section", None),
        ),
        out_specs=(P("section", "dp", None, None), P("section", "dp", None)),
        check_vma=False,
    )
```

```python
import functools
import math

import jax
import jax.numpy as jnp
from jax import lax
from jax.experimental import pallas as pl
from jax.experimental.pallas import tpu as pltpu
from jax.sharding import PartitionSpec as P

epsilon = 1e-05
delta_bound = 2.0
CHUNK = 32
PIECES = 4
Z_UNITS = 7
MESH = pl.DeviceIdType.MESH
f32 = jnp.float32
bf16 = jnp.bfloat16
rsqrt2 = 1.0 / math.sqrt(2.0)
rsqrt2pi = 1.0 / math.sqrt(2.0 * math.pi)


def relay_kernel(
    scale,
    ids_ref, inputs_hbm, stored_hbm, w_hbm, gain_ref,
    out_hbm, wgrad_hbm,
    w_v, wt_v, base_v, keep_v, fin_v, clip_v, normed_v, pre_v, out_v, bin_v,
    mu_v, rs_v, u_v,
    nt_v, ngat_v, nrow_v, gown_v, gz_v, gy_v,
    sem_w, sem_base, sem_keep, fsend, frecv, bsend, brecv, sem_out,
    nsend, nrecv, zsend, zrecv, gsend, grecv, csend, crecv, ysend, yrecv,
    csend2, crecv2, zsend2, zrecv2, sem_res, ready,
):
    s = lax.axis_index("section")
    sections = lax.axis_size("section")
    d = lax.axis_index("dp")
    last = sections - 1
    chunks, rows, width = fin_v.shape
    tokens = base_v.shape[1]
    batches = base_v.shape[0]
    local = chunks * rows
    per_batch = tokens // rows
    block = width // PIECES
    has_next = s < last
    has_prev = s > 0
    nxt = {"section": jnp.minimum(s + 1, last)}
    prv = {"section": jnp.maximum(s - 1, 0)}
    z = d // 4
    rest = d % 4
    core = d % 2
    row = rest // 2
    z_up = (z + 1) % 4
    z_down = (z + 3) % 4
    z_far = (z + 2) % 4
    dev_up = {"dp": z_up * 4 + rest}
    dev_down = {"dp": z_down * 4 + rest}
    dev_far = {"dp": z_far * 4 + rest}
    dev_core = {"dp": d + 1 - 2 * core}
    dev_row = {"dp": z * 4 + (rest + 2) % 4}

    late = s < last - 2

    def w_copy(j):
        cols = pl.ds(pl.multiple_of(j * block, block), block)
        return pltpu.make_async_copy(w_hbm.at[0, :, cols], w_v.at[:, cols], sem_w.at[j])

    @pl.when(s == 0)
    def _():
        pltpu.make_async_copy(inputs_hbm, base_v, sem_base).start()

    @pl.when(has_prev)
    def _():
        pltpu.make_async_copy(stored_hbm.at[0, 0], base_v, sem_base).start()

    for j in range(PIECES):
        w_copy(j).start()
    pltpu.make_async_copy(stored_hbm.at[0, 1], keep_v, sem_keep).start()

    barrier = pltpu.get_barrier_semaphore()

    @pl.when(has_next)
    def _():
        pl.semaphore_signal(barrier, inc=1, device_id=nxt, device_id_type=MESH)

    @pl.when(has_prev)
    def _():
        pl.semaphore_signal(barrier, inc=1, device_id=prv, device_id_type=MESH)

    for peer in (dev_up, dev_down, dev_far, dev_core, dev_row):
        pl.semaphore_signal(barrier, inc=1, device_id=peer, device_id_type=MESH)
    pl.semaphore_wait(barrier, 5 + jnp.minimum(s, 1) + jnp.minimum(last - s, 1))

    @pl.when(s == 0)
    def _():
        fin_v[...] = jnp.zeros_like(fin_v)

    pltpu.make_async_copy(inputs_hbm, base_v, sem_base).wait()
    def prepare():
        side = 256
        line = lax.broadcasted_iota(jnp.int32, (side, side), 0)
        column = lax.broadcasted_iota(jnp.int32, (side, side), 1)
        eye = jnp.where(line == column, 1.0, 0.0).astype(bf16)

        def turn(i, carry):
            cols = pl.ds(pl.multiple_of(i * side, side), side)
            for j in range(PIECES):
                part = pl.ds(j * block, block)
                wt_v[cols, part] = lax.dot_general(
                    eye, w_v[part, cols], (((1,), (1,)), ((), ())), preferred_element_type=f32).astype(bf16)
            return carry

        lax.fori_loop(0, width // side, turn, 0)
        high = gain_ref[...].astype(bf16)
        low = (gain_ref[...] - high.astype(f32)).astype(bf16)
        which = lax.broadcasted_iota(jnp.int32, (16, width), 0)
        pair = jnp.where(which == 0, high.astype(f32), jnp.where(which == 1, low.astype(f32), 0.0)).astype(bf16)

        def weigh(j, carry):
            cols = pl.ds(pl.multiple_of(j * block, block), block)
            both = jnp.dot(pair, w_v[:, cols], preferred_element_type=f32)
            u_v[:, cols] = jnp.broadcast_to(jnp.sum(both, axis=0, keepdims=True), (8, block))
            return carry

        lax.fori_loop(0, PIECES, weigh, 0)

    @pl.when(s == 0)
    def _():
        u_v[...] = jnp.zeros_like(u_v)

    @pl.when(jnp.logical_not(late))
    def _():
        for j in range(PIECES):
            w_copy(j).wait()
        prepare()

    pltpu.make_async_copy(stored_hbm.at[0, 1], keep_v, sem_keep).wait()

    def remote(src, dst, send, recv, device):
        return pltpu.make_async_remote_copy(
            src_ref=src, dst_ref=dst, send_sem=send, recv_sem=recv, device_id=device, device_id_type=MESH)

    def cols_of(j):
        return pl.ds(pl.multiple_of(j * block, block), block)

    def fcopy(c, cols):
        return remote(clip_v.at[c, :, cols], fin_v.at[c, :, cols], fsend.at[c], frecv.at[c], nxt)

    def fwhole(c):
        return remote(clip_v.at[c], fin_v.at[c], fsend.at[c], frecv.at[c], nxt)

    def bcopy(c, j):
        cols = cols_of(j)
        return remote(clip_v.at[c, :, cols], bin_v.at[c, :, cols], bsend.at[c, j], brecv.at[c, j], prv)

    def place(c):
        batch = c // per_batch
        first = pl.multiple_of((c % per_batch) * rows, rows)
        sample = ids_ref[0, batch]
        index = jnp.where(s == 0, batch, sample)
        return batch, first, sample, index

    share = width // 4
    part = share // 4
    unit = width // 12
    split = unit * Z_UNITS
    low_lanes = pl.ds(0, split)
    high_lanes = pl.ds(split, width - split)

    def chunk_rows(c, n=1):
        return pl.ds(pl.multiple_of(c * rows, rows), n * rows)

    def out_copy(c):
        batch, first, sample, index = place(c)
        return pltpu.make_async_copy(out_v.at[c], out_hbm.at[batch, pl.ds(first, rows)], sem_out.at[c])

    circle = ((0, z_up, dev_up), (1, z_down, dev_down), (2, z_far, dev_far))

    def z_copy(c, slot):
        return remote(gown_v.at[chunk_rows(c), low_lanes],
                      gz_v.at[pl.ds(pl.multiple_of(slot * local + c * rows, rows), rows)],
                      zsend.at[slot, c], zrecv.at[slot, c], circle[slot][2])

    def g_copy(c):
        return remote(gown_v.at[chunk_rows(c), high_lanes], gy_v.at[chunk_rows(c)], gsend.at[c], grecv.at[c], dev_row)

    def ncopy(slot):
        return remote(nt_v.at[circle[slot][1]],
                      ngat_v.at[:, pl.ds((slot + 1) * local, local)], nsend.at[slot], nrecv.at[slot], circle[slot][2])

    def nrow_copy():
        return remote(nt_v.at[:, pl.ds(pl.multiple_of((1 - row) * 2 * part, 2 * part), 2 * part)], nrow_v,
                      nsend.at[3], nrecv.at[3], dev_row)

    def share_normed():
        step = share // 3
        def turn(i, carry):
            cols = pl.ds(pl.multiple_of(i * step, step), step)
            for b in range(batches):
                values = normed_v[pl.ds(b * per_batch, per_batch), :, cols].reshape(tokens, step)
                nt_v[i // 3, pl.ds(pl.multiple_of((i % 3) * step, step), step), pl.ds(b * tokens, tokens)] = values.T
            return carry
        lax.fori_loop(0, width // step, turn, 0)
        for slot in range(3):
            ncopy(slot).start()
        nrow_copy().start()
        ngat_v[:, pl.ds(0, local)] = nt_v[z]

    def several(ref, c, n, cols=None):
        if cols is None:
            return ref[pl.ds(c, n)].reshape(n * rows, ref.shape[-1])
        return ref[pl.ds(c, n), :, cols].reshape(n * rows, cols.size)

    def keep(ref, c, n, value, cols=None):
        if cols is None:
            ref[pl.ds(c, n)] = value.reshape(n, rows, value.shape[-1])
        else:
            ref[pl.ds(c, n), :, cols] = value.reshape(n, rows, cols.size)

    def state_of(c, n, cols=None):
        batch, first, sample, index = place(c)
        if cols is None:
            return base_v[index, pl.ds(first, n * rows), :].astype(f32) + several(fin_v, c, n).astype(f32)
        return base_v[index, pl.ds(first, n * rows), cols].astype(f32) + several(fin_v, c, n, cols).astype(f32)

    def forward(c, n, final):
        batch, first, sample, index = place(c)
        if final:
            for i in range(n):
                fwhole(c + i).wait_recv()
        else:
            @pl.when(has_prev)
            def _():
                fwhole(c).wait_recv()

        x = state_of(c, n)
        mu = jnp.mean(x, axis=-1, keepdims=True)
        xc = x - mu
        var = jnp.mean(xc * xc, axis=-1, keepdims=True)
        rs = lax.rsqrt(var + epsilon)
        keep(normed_v, c, n, (xc * rs * gain_ref[...]).astype(bf16))
        keep(mu_v, c, n, jnp.broadcast_to(mu, (n * rows, 128)))
        keep(rs_v, c, n, jnp.broadcast_to(rs, (n * rows, 128)))

        def tile(j, carry2):
            cols = cols_of(j)
            if not final:
                @pl.when(jnp.logical_and(c == 0, late))
                def _():
                    w_copy(j).wait()

            v = jnp.dot(several(normed_v, c, n), w_v[:, cols], preferred_element_type=f32)
            keep(pre_v, c, n, v, cols)
            res = state_of(c, n, cols) + v * (0.5 + 0.5 * lax.erf(v * rsqrt2))
            keep(out_v, c, n, res.astype(bf16), cols)
            if not final:
                kept = keep_v[sample, pl.ds(first, rows), cols].astype(f32)
                clip_v[c, :, cols] = jnp.clip(res - kept, -delta_bound, delta_bound).astype(bf16)
                fcopy(c, cols).start()
            return carry2

        lax.fori_loop(0, PIECES, tile, 0)
        for i in range(n):
            out_copy(c + i).start()

    def backward(c, n, final):
        def piece(j, sums):
            cols = cols_of(j)
            if not final:
                bcopy(c, j).wait_recv()
            v = several(pre_v, c, n, cols)
            cdf = 0.5 + 0.5 * lax.erf(v * rsqrt2)
            slope = cdf + v * (jnp.exp(-0.5 * v * v) * rsqrt2pi)
            if final:
                up = (state_of(c, n, cols) + v * cdf) * scale
            else:
                up = several(bin_v, c, n, cols).astype(f32)
            gp = (slope * up).astype(bf16)
            gown_v[chunk_rows(c, n), cols] = gp
            wide_gp = gp.astype(f32)
            return (
                sums[0] + jnp.sum(wide_gp * u_v[0:1, cols], axis=-1, keepdims=True),
                sums[1] + jnp.sum(wide_gp * v, axis=-1, keepdims=True),
            )

        zero = jnp.zeros((n * rows, 1), f32)
        sums = lax.fori_loop(0, PIECES, piece, (zero, zero))
        for i in range(n):
            for slot in range(3):
                z_copy(c + i, slot).start()

        if not final:
            @pl.when(s == 0)
            def _():
                g_copy(c).start()

        def pull():
            m1 = sums[0] * (1.0 / width)
            m2 = sums[1] * (1.0 / width)
            mu = several(mu_v, c, n)[:, :1]
            rs = several(rs_v, c, n)[:, :1]
            if not final:
                fwhole(c).wait_send()

            def tile(j, carry2):
                cols = cols_of(j)
                gn = jnp.dot(gown_v[chunk_rows(c, n)], wt_v[:, cols], preferred_element_type=f32)
                state = state_of(c, n, cols)
                xhat = (state - mu) * rs
                if final:
                    v = several(pre_v, c, n, cols)
                    up = (state + v * (0.5 + 0.5 * lax.erf(v * rsqrt2))) * scale
                else:
                    up = several(bin_v, c, n, cols).astype(f32)
                sent = up + rs * (gn * gain_ref[:, cols] - m1 - xhat * m2)
                keep(clip_v, c, n, sent.astype(bf16), cols)
                bcopy(c, j).start()
                return carry2

            lax.fori_loop(0, PIECES, tile, 0)
            for i in range(1, n):
                for j in range(PIECES):
                    bcopy(c + i, j).start()

        if final:
            pull()
        else:
            pl.when(has_prev)(pull)

    ahead = jnp.where(s == last - 1, chunks - 2, chunks)

    def step(t, carry):
        @pl.when(t < chunks)
        def _():
            forward(t, 1, False)

        @pl.when(jnp.logical_and(t == chunks - 1, late))
        def _():
            share_normed()

            @pl.when(has_prev)
            def _():
                prepare()

        @pl.when(t >= ahead)
        def _():
            backward(t - ahead, 1, False)

        return carry

    def pair_step(t, carry):
        forward(2 * t, 2, True)

        backward(2 * t, 2, True)
        return carry

    @pl.when(has_next)
    def _():
        lax.fori_loop(0, chunks + ahead, step, 0)

    @pl.when(s == last)
    def _():
        lax.fori_loop(0, chunks // 2, pair_step, 0)

    for peer in (dev_up, dev_down, dev_far, dev_core, dev_row):
        pl.semaphore_signal(ready, inc=1, device_id=peer, device_id_type=MESH)

    def start_rows(c, carry):
        g_copy(c).start()
        return carry

    @pl.when(has_prev)
    def _():
        lax.fori_loop(0, chunks, start_rows, 0)

    @pl.when(jnp.logical_not(late))
    def _():
        share_normed()

    def band(place_of, lanes, count=1):
        return (pl.ds(place_of * part, count * part), lanes)

    def lanes_of(q):
        return pl.ds(pl.multiple_of(q * unit, unit), unit)

    def core_copy(q, y):
        lanes = lanes_of(q)
        return remote(w_v.at[band(y, lanes)], wt_v.at[band(y, lanes)], csend.at[q, y], crecv.at[q, y], dev_core)

    def row_copy(q):
        lanes = lanes_of(q)
        return remote(w_v.at[band(4, lanes)], wt_v.at[band(2, lanes)], ysend.at[q], yrecv.at[q], dev_row)

    def core_copy2(q):
        lanes = lanes_of(q)
        return remote(w_v.at[band(6, lanes, 4)], wt_v.at[band(3, lanes, 4)], csend2.at[q], crecv2.at[q], dev_core)

    def sum_rows(z_of):
        return pl.ds(pl.multiple_of((10 + z_of) * part, part), part)

    def z_copy2(q, slot):
        lanes = lanes_of(q)
        return remote(w_v.at[sum_rows(circle[slot][1]), lanes], wt_v.at[band(7 + slot, lanes)],
                      zsend2.at[slot, q], zrecv2.at[slot, q], circle[slot][2])

    def res_copy(q):
        lanes = lanes_of(q)
        return pltpu.make_async_copy(w_v.at[band(5, lanes)], wgrad_hbm.at[:, lanes], sem_res.at[q])

    def came(c, carry):
        g_copy(c).wait_recv()
        return carry

    lax.fori_loop(0, chunks, came, 0)
    nrow_copy().wait_recv()
    pl.semaphore_wait(ready, 5)

    def high_product(whose, lanes, high):
        mine = nt_v[:, pl.ds(pl.multiple_of(row * 2 * part + whose * part, part), part)].reshape(share, local)
        theirs = nrow_v[:, pl.ds(pl.multiple_of(whose * part, part), part)].reshape(share, local)
        return (
            jnp.dot(mine, gown_v[:, lanes], preferred_element_type=f32)
            + jnp.dot(theirs, gy_v[:, high], preferred_element_type=f32)
        ).astype(bf16)

    def product2(q, carry):
        @pl.when(q < 12)
        def _():
            lanes = lanes_of(q)
            high = pl.ds(pl.multiple_of((q - Z_UNITS) * unit, unit), unit)
            w_v[band(6, lanes, 4)] = high_product(1 - core, lanes, high)
            core_copy2(q).start()
            w_v[band(10, lanes, 4)] = high_product(core, lanes, high)

        @pl.when(q > Z_UNITS)
        def _():
            lanes = lanes_of(q - 1)
            core_copy2(q - 1).wait_recv()
            w_v[band(10, lanes, 4)] = (
                w_v[band(10, lanes, 4)].astype(f32) + wt_v[band(3, lanes, 4)].astype(f32)
            ).astype(bf16)
            for slot in range(3):
                z_copy2(q - 1, slot).start()

        return carry

    lax.fori_loop(Z_UNITS, 13, product2, 0)

    def arrived(c, carry):
        for slot in range(3):
            z_copy(c, slot).wait_recv()
        return carry

    for slot in range(3):
        ncopy(slot).wait_recv()
    lax.fori_loop(0, chunks, arrived, 0)

    def low_product(y, whose, lanes):
        lines = pl.ds(pl.multiple_of(y * 2 * part + whose * part, part), part)
        return (
            jnp.dot(ngat_v[lines, pl.ds(0, local)], gown_v[:, lanes], preferred_element_type=f32)
            + jnp.dot(ngat_v[lines, pl.ds(local, 3 * local)], gz_v[:, lanes], preferred_element_type=f32)
        ).astype(bf16)

    def one_of(first, which):
        return pl.ds(pl.multiple_of((first + which) * part, part), part)

    def product(q, carry):
        @pl.when(q < Z_UNITS)
        def _():
            lanes = lanes_of(q)
            for y in range(2):
                w_v[band(y, lanes)] = low_product(y, 1 - core, lanes)
                core_copy(q, y).start()
            for y in range(2):
                w_v[band(2 + y, lanes)] = low_product(y, core, lanes)

        @pl.when(q >= 1)
        def _():
            lanes = lanes_of(q - 1)
            for y in range(2):
                core_copy(q - 1, y).wait_recv()
            w_v[band(4, lanes)] = (
                w_v[one_of(2, 1 - row), lanes].astype(f32) + wt_v[one_of(0, 1 - row), lanes].astype(f32)
            ).astype(bf16)
            row_copy(q - 1).start()

        return carry

    lax.fori_loop(0, Z_UNITS + 1, product, 0)

    def total2(q, carry):
        lanes = lanes_of(q)
        result = w_v[sum_rows(z), lanes].astype(f32)
        for slot in range(3):
            z_copy2(q, slot).wait_recv()
            result += wt_v[band(7 + slot, lanes)].astype(f32)
        w_v[band(5, lanes)] = result.astype(bf16)
        res_copy(q).start()
        return carry

    def total(q, carry):
        lanes = lanes_of(q)
        row_copy(q).wait_recv()
        w_v[band(5, lanes)] = (
            w_v[one_of(2, row), lanes].astype(f32) + wt_v[one_of(0, row), lanes].astype(f32)
            + wt_v[band(2, lanes)].astype(f32)
        ).astype(bf16)
        res_copy(q).start()
        return carry

    lax.fori_loop(Z_UNITS, 12, total2, 0)
    lax.fori_loop(0, Z_UNITS, total, 0)

    def finish(c, carry):
        out_copy(c).wait()
        g_copy(c).wait_send()
        for slot in range(3):
            z_copy(c, slot).wait_send()

        @pl.when(s == 0)
        def _():
            fwhole(c).wait_send()

        @pl.when(has_prev)
        def _():
            for j in range(PIECES):
                bcopy(c, j).wait_send()

        return carry

    lax.fori_loop(0, chunks, finish, 0)

    def finish_low(q, carry):
        for y in range(2):
            core_copy(q, y).wait_send()
        row_copy(q).wait_send()
        res_copy(q).wait()
        return carry

    def finish_high(q, carry):
        core_copy2(q).wait_send()
        for slot in range(3):
            z_copy2(q, slot).wait_send()
        res_copy(q).wait()
        return carry

    lax.fori_loop(0, Z_UNITS, finish_low, 0)
    lax.fori_loop(Z_UNITS, 12, finish_high, 0)
    for slot in range(3):
        ncopy(slot).wait_send()
    nrow_copy().wait_send()


def relay(scale, inputs, sample_ids, stored, weight, norm_gain):
    batches, tokens, width = inputs.shape
    rows = min(CHUNK, tokens)
    local = batches * tokens
    chunks = local // rows
    share = width // 4
    part = share // 4
    split = width // 12 * Z_UNITS
    any_spec = pl.BlockSpec(memory_space=pl.ANY)
    chunked = pltpu.VMEM((chunks, rows, width), bf16)
    dma = pltpu.SemaphoreType.DMA
    return pl.pallas_call(
        functools.partial(relay_kernel, scale),
        out_shape=(
            jax.ShapeDtypeStruct(inputs.shape, bf16),
            jax.ShapeDtypeStruct((part, width), bf16),
        ),
        in_specs=[
            pl.BlockSpec(memory_space=pltpu.SMEM), any_spec, any_spec, any_spec,
            pl.BlockSpec(memory_space=pltpu.VMEM),
        ],
        out_specs=(any_spec, any_spec),
        scratch_shapes=[
            pltpu.VMEM((width, width), bf16),
            pltpu.VMEM((width, width), bf16),
            pltpu.VMEM(inputs.shape, bf16),
            pltpu.VMEM(inputs.shape, bf16),
            chunked, chunked, chunked,
            pltpu.VMEM((chunks, rows, width), f32),
            chunked, chunked,
            pltpu.VMEM((chunks, rows, 128), f32),
            pltpu.VMEM((chunks, rows, 128), f32),
            pltpu.VMEM((8, width), f32),
            pltpu.VMEM((4, share, local), bf16),
            pltpu.VMEM((share, 4 * local), bf16),
            pltpu.VMEM((4, 2 * part, local), bf16),
            pltpu.VMEM((local, width), bf16),
            pltpu.VMEM((3 * local, split), bf16),
            pltpu.VMEM((local, width - split), bf16),
            dma((PIECES,)), dma, dma,
            dma((chunks,)), dma((chunks,)),
            dma((chunks, PIECES)), dma((chunks, PIECES)),
            dma((chunks,)),
            dma((4,)), dma((4,)),
            dma((3, chunks)), dma((3, chunks)),
            dma((chunks,)), dma((chunks,)),
            dma((Z_UNITS, 2)), dma((Z_UNITS, 2)),
            dma((Z_UNITS,)), dma((Z_UNITS,)),
            dma((12,)), dma((12,)),
            dma((3, 12)), dma((3, 12)),
            dma((12,)), pltpu.SemaphoreType.REGULAR,
        ],
        compiler_params=pltpu.CompilerParams(
            collective_id=0, has_side_effects=True, vmem_limit_bytes=67043328),
        cost_estimate=pl.CostEstimate(
            flops=6 * local * width * width, bytes_accessed=2 * width * width, transcendentals=0),
        name="relay",
    )(sample_ids, inputs, stored, weight, norm_gain)


def per_device(inputs, sample_ids, stored, weight, norm_gain):
    batches, tokens, width = inputs.shape
    scale = 1.0 / math.sqrt(lax.axis_size("dp") * batches * tokens)
    outs, summed = relay(scale, inputs, sample_ids, stored, weight, norm_gain)
    return (outs[None], summed[None])


def solution(mesh):
    return jax.shard_map(
        per_device,
        mesh=mesh,
        in_specs=(
            P("dp", None, None),
            P("dp", None),
            P("section", None, "dp", None, None),
            P("section", None, None),
            P("section", None),
        ),
        out_specs=(P("section", "dp", None, None), P("section", "dp", None)),
        check_vma=False,
    )
```

```python
import functools
import math

import jax
import jax.numpy as jnp
from jax import lax
from jax.experimental import pallas as pl
from jax.experimental.pallas import tpu as pltpu
from jax.sharding import PartitionSpec as P

epsilon = 1e-05
delta_bound = 2.0
CHUNK = 32
PIECES = 4
Z_UNITS = 7
LAG = 2
MESH = pl.DeviceIdType.MESH
f32 = jnp.float32
bf16 = jnp.bfloat16
rsqrt2 = 1.0 / math.sqrt(2.0)
rsqrt2pi = 1.0 / math.sqrt(2.0 * math.pi)


def relay_kernel(
    scale,
    ids_ref, inputs_hbm, stored_hbm, w_hbm, gain_ref,
    out_hbm, wgrad_hbm,
    w_v, wt_v, base_v, keep_v, fin_v, clip_v, normed_v, pre_v, slope_v, out_v, bin_v,
    mu_v, rs_v, u_v,
    nt_v, ngat_v, nrow_v, gown_v, gz_v, gy_v,
    sem_w, sem_base, sem_keep, fsend, frecv, bsend, brecv, sem_out,
    nsend, nrecv, zsend, zrecv, gsend, grecv, csend, crecv, ysend, yrecv,
    csend2, crecv2, zsend2, zrecv2, sem_res, ready,
):
    s = lax.axis_index("section")
    sections = lax.axis_size("section")
    d = lax.axis_index("dp")
    last = sections - 1
    chunks, rows, width = fin_v.shape
    tokens = base_v.shape[1]
    batches = base_v.shape[0]
    local = chunks * rows
    per_batch = tokens // rows
    block = width // PIECES
    has_next = s < last
    has_prev = s > 0
    nxt = {"section": jnp.minimum(s + 1, last)}
    prv = {"section": jnp.maximum(s - 1, 0)}
    z = d // 4
    rest = d % 4
    core = d % 2
    row = rest // 2
    z_up = (z + 1) % 4
    z_down = (z + 3) % 4
    z_far = (z + 2) % 4
    dev_up = {"dp": z_up * 4 + rest}
    dev_down = {"dp": z_down * 4 + rest}
    dev_far = {"dp": z_far * 4 + rest}
    dev_core = {"dp": d + 1 - 2 * core}
    dev_row = {"dp": z * 4 + (rest + 2) % 4}

    late = s < last - 2

    def w_copy(j):
        cols = pl.ds(pl.multiple_of(j * block, block), block)
        return pltpu.make_async_copy(w_hbm.at[0, :, cols], w_v.at[:, cols], sem_w.at[j])

    @pl.when(s == 0)
    def _():
        pltpu.make_async_copy(inputs_hbm, base_v, sem_base).start()

    @pl.when(has_prev)
    def _():
        pltpu.make_async_copy(stored_hbm.at[0, 0], base_v, sem_base).start()

    for j in range(PIECES):
        w_copy(j).start()
    pltpu.make_async_copy(stored_hbm.at[0, 1], keep_v, sem_keep).start()

    barrier = pltpu.get_barrier_semaphore()

    @pl.when(has_next)
    def _():
        pl.semaphore_signal(barrier, inc=1, device_id=nxt, device_id_type=MESH)

    @pl.when(has_prev)
    def _():
        pl.semaphore_signal(barrier, inc=1, device_id=prv, device_id_type=MESH)

    for peer in (dev_up, dev_down, dev_far, dev_core, dev_row):
        pl.semaphore_signal(barrier, inc=1, device_id=peer, device_id_type=MESH)
    pl.semaphore_wait(barrier, 5 + jnp.minimum(s, 1) + jnp.minimum(last - s, 1))

    @pl.when(s == 0)
    def _():
        fin_v[...] = jnp.zeros_like(fin_v)

    pltpu.make_async_copy(inputs_hbm, base_v, sem_base).wait()
    def prepare():
        side = 256
        line = lax.broadcasted_iota(jnp.int32, (side, side), 0)
        column = lax.broadcasted_iota(jnp.int32, (side, side), 1)
        eye = jnp.where(line == column, 1.0, 0.0).astype(bf16)

        def turn(i, carry):
            cols = pl.ds(pl.multiple_of(i * side, side), side)
            for j in range(PIECES):
                part = pl.ds(j * block, block)
                wt_v[cols, part] = lax.dot_general(
                    eye, w_v[part, cols], (((1,), (1,)), ((), ())), preferred_element_type=f32).astype(bf16)
            return carry

        lax.fori_loop(0, width // side, turn, 0)
        high = gain_ref[...].astype(bf16)
        low = (gain_ref[...] - high.astype(f32)).astype(bf16)
        which = lax.broadcasted_iota(jnp.int32, (16, width), 0)
        pair = jnp.where(which == 0, high.astype(f32), jnp.where(which == 1, low.astype(f32), 0.0)).astype(bf16)

        def weigh(j, carry):
            cols = pl.ds(pl.multiple_of(j * block, block), block)
            both = jnp.dot(pair, w_v[:, cols], preferred_element_type=f32)
            u_v[:, cols] = jnp.broadcast_to(jnp.sum(both, axis=0, keepdims=True), (8, block))
            return carry

        lax.fori_loop(0, PIECES, weigh, 0)

    @pl.when(s == 0)
    def _():
        u_v[...] = jnp.zeros_like(u_v)

    @pl.when(jnp.logical_not(late))
    def _():
        for j in range(PIECES):
            w_copy(j).wait()
        prepare()

    pltpu.make_async_copy(stored_hbm.at[0, 1], keep_v, sem_keep).wait()

    def remote(src, dst, send, recv, device):
        return pltpu.make_async_remote_copy(
            src_ref=src, dst_ref=dst, send_sem=send, recv_sem=recv, device_id=device, device_id_type=MESH)

    def cols_of(j):
        return pl.ds(pl.multiple_of(j * block, block), block)

    def fcopy(c, cols):
        return remote(clip_v.at[c, :, cols], fin_v.at[c, :, cols], fsend.at[c], frecv.at[c], nxt)

    def fwhole(c):
        return remote(clip_v.at[c], fin_v.at[c], fsend.at[c], frecv.at[c], nxt)

    def bcopy(c, j):
        cols = cols_of(j)
        return remote(clip_v.at[c, :, cols], bin_v.at[c, :, cols], bsend.at[c, j], brecv.at[c, j], prv)

    def place(c):
        batch = c // per_batch
        first = pl.multiple_of((c % per_batch) * rows, rows)
        sample = ids_ref[0, batch]
        index = jnp.where(s == 0, batch, sample)
        return batch, first, sample, index

    share = width // 4
    part = share // 4
    unit = width // 12
    split = unit * Z_UNITS
    low_lanes = pl.ds(0, split)
    high_lanes = pl.ds(split, width - split)

    def chunk_rows(c, n=1):
        return pl.ds(pl.multiple_of(c * rows, rows), n * rows)

    def out_copy(c):
        batch, first, sample, index = place(c)
        return pltpu.make_async_copy(out_v.at[c], out_hbm.at[batch, pl.ds(first, rows)], sem_out.at[c])

    circle = ((0, z_up, dev_up), (1, z_down, dev_down), (2, z_far, dev_far))

    def z_copy(c, slot):
        return remote(gown_v.at[chunk_rows(c), low_lanes],
                      gz_v.at[pl.ds(pl.multiple_of(slot * local + c * rows, rows), rows)],
                      zsend.at[slot, c], zrecv.at[slot, c], circle[slot][2])

    def g_copy(c):
        return remote(gown_v.at[chunk_rows(c), high_lanes], gy_v.at[chunk_rows(c)], gsend.at[c], grecv.at[c], dev_row)

    def ncopy(slot):
        return remote(nt_v.at[circle[slot][1]],
                      ngat_v.at[:, pl.ds((slot + 1) * local, local)], nsend.at[slot], nrecv.at[slot], circle[slot][2])

    def nrow_copy():
        return remote(nt_v.at[:, pl.ds(pl.multiple_of((1 - row) * 2 * part, 2 * part), 2 * part)], nrow_v,
                      nsend.at[3], nrecv.at[3], dev_row)

    def share_normed():
        step = share // 3
        def turn(i, carry):
            cols = pl.ds(pl.multiple_of(i * step, step), step)
            for b in range(batches):
                values = normed_v[pl.ds(b * per_batch, per_batch), :, cols].reshape(tokens, step)
                nt_v[i // 3, pl.ds(pl.multiple_of((i % 3) * step, step), step), pl.ds(b * tokens, tokens)] = values.T
            return carry
        lax.fori_loop(0, width // step, turn, 0)
        for slot in range(3):
            ncopy(slot).start()
        nrow_copy().start()
        ngat_v[:, pl.ds(0, local)] = nt_v[z]

    def several(ref, c, n, cols=None):
        if cols is None:
            return ref[pl.ds(c, n)].reshape(n * rows, ref.shape[-1])
        return ref[pl.ds(c, n), :, cols].reshape(n * rows, cols.size)

    def keep(ref, c, n, value, cols=None):
        if cols is None:
            ref[pl.ds(c, n)] = value.reshape(n, rows, value.shape[-1])
        else:
            ref[pl.ds(c, n), :, cols] = value.reshape(n, rows, cols.size)

    def state_of(c, n, cols=None):
        batch, first, sample, index = place(c)
        if cols is None:
            return base_v[index, pl.ds(first, n * rows), :].astype(f32) + several(fin_v, c, n).astype(f32)
        return base_v[index, pl.ds(first, n * rows), cols].astype(f32) + several(fin_v, c, n, cols).astype(f32)

    def forward(c, n, final):
        batch, first, sample, index = place(c)
        if final:
            for i in range(n):
                fwhole(c + i).wait_recv()
        else:
            @pl.when(has_prev)
            def _():
                fwhole(c).wait_recv()

        x = state_of(c, n)
        mu = jnp.mean(x, axis=-1, keepdims=True)
        xc = x - mu
        var = jnp.mean(xc * xc, axis=-1, keepdims=True)
        rs = lax.rsqrt(var + epsilon)
        keep(normed_v, c, n, (xc * rs * gain_ref[...]).astype(bf16))
        keep(mu_v, c, n, jnp.broadcast_to(mu, (n * rows, 128)))
        keep(rs_v, c, n, jnp.broadcast_to(rs, (n * rows, 128)))

        pieces = 2 * PIECES if final else PIECES
        narrow = width // pieces

        def tile(j, carry2):
            cols = pl.ds(pl.multiple_of(j * narrow, narrow), narrow)
            if not final:
                @pl.when(jnp.logical_and(c == 0, late))
                def _():
                    w_copy(j).wait()

            v = jnp.dot(several(normed_v, c, n), w_v[:, cols], preferred_element_type=f32)
            cdf = 0.5 + 0.5 * lax.erf(v * rsqrt2)
            res = state_of(c, n, cols) + v * cdf
            keep(out_v, c, n, res.astype(bf16), cols)
            if not final:
                kept = keep_v[sample, pl.ds(first, rows), cols].astype(f32)
                clip_v[c, :, cols] = jnp.clip(res - kept, -delta_bound, delta_bound).astype(bf16)
                fcopy(c, cols).start()
                keep(pre_v, c, n, v, cols)
            slope = cdf + v * (jnp.exp(-0.5 * v * v) * rsqrt2pi)
            if not final:
                keep(slope_v, c, n, slope.astype(bf16), cols)
                return carry2
            up = res * scale
            keep(pre_v, 0, n, up, cols)
            return push_back(c, n, cols, slope * up, v, carry2)

        zero = jnp.zeros((n * rows, 1), f32)
        sums = lax.fori_loop(0, pieces, tile, (zero, zero) if final else 0)
        for i in range(n):
            out_copy(c + i).start()
        return sums

    def push_back(c, n, cols, value, v, sums):
        gp = value.astype(bf16)
        gown_v[chunk_rows(c, n), cols] = gp
        wide_gp = gp.astype(f32)
        return (
            sums[0] + jnp.sum(wide_gp * u_v[0:1, cols], axis=-1, keepdims=True),
            sums[1] + jnp.sum(wide_gp * v, axis=-1, keepdims=True),
        )

    def backward(c, n, sums):
        final = sums is not None

        def piece(j, sums):
            cols = cols_of(j)
            bcopy(c, j).wait_recv()
            up = several(bin_v, c, n, cols).astype(f32)
            return push_back(c, n, cols, several(slope_v, c, n, cols).astype(f32) * up, several(pre_v, c, n, cols), sums)

        if not final:
            zero = jnp.zeros((n * rows, 1), f32)
            sums = lax.fori_loop(0, PIECES, piece, (zero, zero))
        for i in range(n):
            for slot in range(3):
                z_copy(c + i, slot).start()

        if not final:
            @pl.when(s == 0)
            def _():
                g_copy(c).start()

        def pull():
            m1 = sums[0] * (1.0 / width)
            m2 = sums[1] * (1.0 / width)
            mu = several(mu_v, c, n)[:, :1]
            rs = several(rs_v, c, n)[:, :1]
            if not final:
                fwhole(c).wait_send()

            def tile(j, carry2):
                cols = cols_of(j)
                gn = jnp.dot(gown_v[chunk_rows(c, n)], wt_v[:, cols], preferred_element_type=f32)
                state = state_of(c, n, cols)
                xhat = (state - mu) * rs
                if final:
                    up = several(pre_v, 0, n, cols)
                else:
                    up = several(bin_v, c, n, cols).astype(f32)
                sent = up + rs * (gn * gain_ref[:, cols] - m1 - xhat * m2)
                keep(clip_v, c, n, sent.astype(bf16), cols)
                bcopy(c, j).start()
                return carry2

            lax.fori_loop(0, PIECES, tile, 0)
            for i in range(1, n):
                for j in range(PIECES):
                    bcopy(c + i, j).start()

        if final:
            pull()
        else:
            pl.when(has_prev)(pull)

    def forward_step(c, carry):
        forward(c, 1, False)
        return carry

    def backward_step(c, carry):
        backward(c, 1, None)
        return carry

    def pair_step(t, carry):
        sums = forward(2 * t, 2, True)

        backward(2 * t, 2, sums)
        return carry

    @pl.when(has_next)
    def _():
        lax.fori_loop(0, chunks, forward_step, 0)

        @pl.when(late)
        def _():
            share_normed()

            @pl.when(has_prev)
            def _():
                prepare()

        lax.fori_loop(0, chunks, backward_step, 0)

    @pl.when(s == last)
    def _():
        lax.fori_loop(0, chunks // 2, pair_step, 0)

    for peer in (dev_up, dev_down, dev_far, dev_core, dev_row):
        pl.semaphore_signal(ready, inc=1, device_id=peer, device_id_type=MESH)

    def start_rows(c, carry):
        g_copy(c).start()
        return carry

    @pl.when(has_prev)
    def _():
        lax.fori_loop(0, chunks, start_rows, 0)

    @pl.when(jnp.logical_not(late))
    def _():
        share_normed()

    def band(place_of, lanes, count=1):
        return (pl.ds(place_of * part, count * part), lanes)

    def lanes_of(q):
        return pl.ds(pl.multiple_of(q * unit, unit), unit)

    def core_copy(q, y):
        lanes = lanes_of(q)
        return remote(w_v.at[band(y, lanes)], wt_v.at[band(y, lanes)], csend.at[q, y], crecv.at[q, y], dev_core)

    def row_copy(q):
        lanes = lanes_of(q)
        return remote(w_v.at[band(4, lanes)], wt_v.at[band(2, lanes)], ysend.at[q], yrecv.at[q], dev_row)

    def core_copy2(q):
        lanes = lanes_of(q)
        return remote(w_v.at[band(6, lanes, 4)], wt_v.at[band(3, lanes, 4)], csend2.at[q], crecv2.at[q], dev_core)

    def sum_rows(z_of):
        return pl.ds(pl.multiple_of((10 + z_of) * part, part), part)

    def z_copy2(q, slot):
        lanes = lanes_of(q)
        return remote(w_v.at[sum_rows(circle[slot][1]), lanes], wt_v.at[band(7 + slot, lanes)],
                      zsend2.at[slot, q], zrecv2.at[slot, q], circle[slot][2])

    def res_copy(q):
        lanes = lanes_of(q)
        return pltpu.make_async_copy(w_v.at[band(5, lanes)], wgrad_hbm.at[:, lanes], sem_res.at[q])

    def came(c, carry):
        g_copy(c).wait_recv()
        return carry

    lax.fori_loop(0, chunks, came, 0)
    nrow_copy().wait_recv()
    pl.semaphore_wait(ready, 5)

    def high_product(whose, lanes, high):
        mine = nt_v[:, pl.ds(pl.multiple_of(row * 2 * part + whose * part, part), part)].reshape(share, local)
        theirs = nrow_v[:, pl.ds(pl.multiple_of(whose * part, part), part)].reshape(share, local)
        return (
            jnp.dot(mine, gown_v[:, lanes], preferred_element_type=f32)
            + jnp.dot(theirs, gy_v[:, high], preferred_element_type=f32)
        ).astype(bf16)

    def product2(q, carry):
        @pl.when(q < 12)
        def _():
            lanes = lanes_of(q)
            high = pl.ds(pl.multiple_of((q - Z_UNITS) * unit, unit), unit)
            w_v[band(6, lanes, 4)] = high_product(1 - core, lanes, high)
            core_copy2(q).start()
            w_v[band(10, lanes, 4)] = high_product(core, lanes, high)

        @pl.when(q >= Z_UNITS + LAG)
        def _():
            lanes = lanes_of(q - LAG)
            core_copy2(q - LAG).wait_recv()
            w_v[band(10, lanes, 4)] = (
                w_v[band(10, lanes, 4)].astype(f32) + wt_v[band(3, lanes, 4)].astype(f32)
            ).astype(bf16)
            for slot in range(3):
                z_copy2(q - LAG, slot).start()

        return carry

    lax.fori_loop(Z_UNITS, 12 + LAG, product2, 0)

    def arrived(c, carry):
        for slot in range(3):
            z_copy(c, slot).wait_recv()
        return carry

    for slot in range(3):
        ncopy(slot).wait_recv()
    lax.fori_loop(0, chunks, arrived, 0)

    def low_product(y, whose, lanes):
        lines = pl.ds(pl.multiple_of(y * 2 * part + whose * part, part), part)
        return (
            jnp.dot(ngat_v[lines, pl.ds(0, local)], gown_v[:, lanes], preferred_element_type=f32)
            + jnp.dot(ngat_v[lines, pl.ds(local, 3 * local)], gz_v[:, lanes], preferred_element_type=f32)
        ).astype(bf16)

    def one_of(first, which):
        return pl.ds(pl.multiple_of((first + which) * part, part), part)

    def product(q, carry):
        @pl.when(q < Z_UNITS)
        def _():
            lanes = lanes_of(q)
            for y in range(2):
                w_v[band(y, lanes)] = low_product(y, 1 - core, lanes)
                core_copy(q, y).start()
            for y in range(2):
                w_v[band(2 + y, lanes)] = low_product(y, core, lanes)

        @pl.when(q >= LAG)
        def _():
            lanes = lanes_of(q - LAG)
            for y in range(2):
                core_copy(q - LAG, y).wait_recv()
            w_v[band(4, lanes)] = (
                w_v[one_of(2, 1 - row), lanes].astype(f32) + wt_v[one_of(0, 1 - row), lanes].astype(f32)
            ).astype(bf16)
            row_copy(q - LAG).start()

        return carry

    lax.fori_loop(0, Z_UNITS + LAG, product, 0)

    def total2(q, carry):
        lanes = lanes_of(q)
        result = w_v[sum_rows(z), lanes].astype(f32)
        for slot in range(3):
            z_copy2(q, slot).wait_recv()
            result += wt_v[band(7 + slot, lanes)].astype(f32)
        w_v[band(5, lanes)] = result.astype(bf16)
        res_copy(q).start()
        return carry

    def total(q, carry):
        lanes = lanes_of(q)
        row_copy(q).wait_recv()
        w_v[band(5, lanes)] = (
            w_v[one_of(2, row), lanes].astype(f32) + wt_v[one_of(0, row), lanes].astype(f32)
            + wt_v[band(2, lanes)].astype(f32)
        ).astype(bf16)
        res_copy(q).start()
        return carry

    lax.fori_loop(Z_UNITS, 12, total2, 0)
    lax.fori_loop(0, Z_UNITS, total, 0)

    def finish(c, carry):
        out_copy(c).wait()
        g_copy(c).wait_send()
        for slot in range(3):
            z_copy(c, slot).wait_send()

        @pl.when(s == 0)
        def _():
            fwhole(c).wait_send()

        @pl.when(has_prev)
        def _():
            for j in range(PIECES):
                bcopy(c, j).wait_send()

        return carry

    lax.fori_loop(0, chunks, finish, 0)

    def finish_low(q, carry):
        for y in range(2):
            core_copy(q, y).wait_send()
        row_copy(q).wait_send()
        res_copy(q).wait()
        return carry

    def finish_high(q, carry):
        core_copy2(q).wait_send()
        for slot in range(3):
            z_copy2(q, slot).wait_send()
        res_copy(q).wait()
        return carry

    lax.fori_loop(0, Z_UNITS, finish_low, 0)
    lax.fori_loop(Z_UNITS, 12, finish_high, 0)
    for slot in range(3):
        ncopy(slot).wait_send()
    nrow_copy().wait_send()


def relay(scale, inputs, sample_ids, stored, weight, norm_gain):
    batches, tokens, width = inputs.shape
    rows = min(CHUNK, tokens)
    local = batches * tokens
    chunks = local // rows
    share = width // 4
    part = share // 4
    split = width // 12 * Z_UNITS
    any_spec = pl.BlockSpec(memory_space=pl.ANY)
    chunked = pltpu.VMEM((chunks, rows, width), bf16)
    dma = pltpu.SemaphoreType.DMA
    return pl.pallas_call(
        functools.partial(relay_kernel, scale),
        out_shape=(
            jax.ShapeDtypeStruct(inputs.shape, bf16),
            jax.ShapeDtypeStruct((part, width), bf16),
        ),
        in_specs=[
            pl.BlockSpec(memory_space=pltpu.SMEM), any_spec, any_spec, any_spec,
            pl.BlockSpec(memory_space=pltpu.VMEM),
        ],
        out_specs=(any_spec, any_spec),
        scratch_shapes=[
            pltpu.VMEM((width, width), bf16),
            pltpu.VMEM((width, width), bf16),
            pltpu.VMEM(inputs.shape, bf16),
            pltpu.VMEM(inputs.shape, bf16),
            chunked, chunked, chunked,
            pltpu.VMEM((chunks, rows, width), f32),
            chunked, chunked, chunked,
            pltpu.VMEM((chunks, rows, 128), f32),
            pltpu.VMEM((chunks, rows, 128), f32),
            pltpu.VMEM((8, width), f32),
            pltpu.VMEM((4, share, local), bf16),
            pltpu.VMEM((share, 4 * local), bf16),
            pltpu.VMEM((4, 2 * part, local), bf16),
            pltpu.VMEM((local, width), bf16),
            pltpu.VMEM((3 * local, split), bf16),
            pltpu.VMEM((local, width - split), bf16),
            dma((PIECES,)), dma, dma,
            dma((chunks,)), dma((chunks,)),
            dma((chunks, PIECES)), dma((chunks, PIECES)),
            dma((chunks,)),
            dma((4,)), dma((4,)),
            dma((3, chunks)), dma((3, chunks)),
            dma((chunks,)), dma((chunks,)),
            dma((Z_UNITS, 2)), dma((Z_UNITS, 2)),
            dma((Z_UNITS,)), dma((Z_UNITS,)),
            dma((12,)), dma((12,)),
            dma((3, 12)), dma((3, 12)),
            dma((12,)), pltpu.SemaphoreType.REGULAR,
        ],
        compiler_params=pltpu.CompilerParams(
            collective_id=0, has_side_effects=True, vmem_limit_bytes=67043328),
        cost_estimate=pl.CostEstimate(
            flops=6 * local * width * width, bytes_accessed=2 * width * width, transcendentals=0),
        name="relay",
    )(sample_ids, inputs, stored, weight, norm_gain)


def per_device(inputs, sample_ids, stored, weight, norm_gain):
    batches, tokens, width = inputs.shape
    scale = 1.0 / math.sqrt(lax.axis_size("dp") * batches * tokens)
    outs, summed = relay(scale, inputs, sample_ids, stored, weight, norm_gain)
    return (outs[None], summed[None])


def solution(mesh):
    return jax.shard_map(
        per_device,
        mesh=mesh,
        in_specs=(
            P("dp", None, None),
            P("dp", None),
            P("section", None, "dp", None, None),
            P("section", None, None),
            P("section", None),
        ),
        out_specs=(P("section", "dp", None, None), P("section", "dp", None)),
        check_vma=False,
    )
```

```python
import functools
import math

import jax
import jax.numpy as jnp
from jax import lax
from jax.experimental import pallas as pl
from jax.experimental.pallas import tpu as pltpu
from jax.sharding import PartitionSpec as P

epsilon = 1e-05
delta_bound = 2.0
CHUNK = 32
PIECES = 4
Z_UNITS = 7
VMEM_LIMIT = 64200000
LAG = 2
NEAR_LAG = 6
MESH = pl.DeviceIdType.MESH
f32 = jnp.float32
bf16 = jnp.bfloat16
rsqrt2 = 1.0 / math.sqrt(2.0)
rsqrt2pi = 1.0 / math.sqrt(2.0 * math.pi)


def relay_kernel(
    scale,
    ids_ref, inputs_hbm, stored_hbm, w_hbm, gain_ref,
    out_v, wgrad_v,
    w_v, wt_v, base_v, keep_v, fin_v, clip_v, normed_v, pre_v, slope_v, bin_v,
    mu_v, rs_v, u_v,
    nt_v, ngat_v, nrow_v, gown_v, gz_v, gy_v,
    sem_w, sem_base, sem_keep, fsend, frecv, bsend, brecv,
    nsend, nrecv, zsend, zrecv, gsend, grecv, csend, crecv, ysend, yrecv,
    csend2, crecv2, zsend2, zrecv2, ready,
):
    s = lax.axis_index("section")
    sections = lax.axis_size("section")
    d = lax.axis_index("dp")
    last = sections - 1
    chunks, rows, width = fin_v.shape
    tokens = base_v.shape[1]
    batches = base_v.shape[0]
    local = chunks * rows
    per_batch = tokens // rows
    block = width // PIECES
    has_next = s < last
    has_prev = s > 0
    nxt = {"section": jnp.minimum(s + 1, last)}
    prv = {"section": jnp.maximum(s - 1, 0)}
    z = d // 4
    rest = d % 4
    core = d % 2
    row = rest // 2
    z_up = (z + 1) % 4
    z_down = (z + 3) % 4
    z_far = (z + 2) % 4
    dev_up = {"dp": z_up * 4 + rest}
    dev_down = {"dp": z_down * 4 + rest}
    dev_far = {"dp": z_far * 4 + rest}
    dev_core = {"dp": d + 1 - 2 * core}
    dev_row = {"dp": z * 4 + (rest + 2) % 4}

    late = s < last - 2

    def w_copy(j):
        cols = pl.ds(pl.multiple_of(j * block, block), block)
        return pltpu.make_async_copy(w_hbm.at[0, :, cols], w_v.at[:, cols], sem_w.at[j])

    @pl.when(s == 0)
    def _():
        pltpu.make_async_copy(inputs_hbm, base_v, sem_base).start()

    @pl.when(has_prev)
    def _():
        pltpu.make_async_copy(stored_hbm.at[0, 0], base_v, sem_base).start()

    for j in range(PIECES):
        w_copy(j).start()
    pltpu.make_async_copy(stored_hbm.at[0, 1], keep_v, sem_keep).start()

    barrier = pltpu.get_barrier_semaphore()

    @pl.when(has_next)
    def _():
        pl.semaphore_signal(barrier, inc=1, device_id=nxt, device_id_type=MESH)

    @pl.when(has_prev)
    def _():
        pl.semaphore_signal(barrier, inc=1, device_id=prv, device_id_type=MESH)

    for peer in (dev_up, dev_down, dev_far, dev_core, dev_row):
        pl.semaphore_signal(barrier, inc=1, device_id=peer, device_id_type=MESH)
    pl.semaphore_wait(barrier, 5 + jnp.minimum(s, 1) + jnp.minimum(last - s, 1))

    @pl.when(s == 0)
    def _():
        fin_v[...] = jnp.zeros_like(fin_v)

    pltpu.make_async_copy(inputs_hbm, base_v, sem_base).wait()
    def prepare():
        side = 256
        line = lax.broadcasted_iota(jnp.int32, (side, side), 0)
        column = lax.broadcasted_iota(jnp.int32, (side, side), 1)
        eye = jnp.where(line == column, 1.0, 0.0).astype(bf16)

        def turn(i, carry):
            cols = pl.ds(pl.multiple_of(i * side, side), side)
            for j in range(PIECES):
                part = pl.ds(j * block, block)
                wt_v[cols, part] = lax.dot_general(
                    eye, w_v[part, cols], (((1,), (1,)), ((), ())), preferred_element_type=f32).astype(bf16)
            return carry

        lax.fori_loop(0, width // side, turn, 0)
        high = gain_ref[...].astype(bf16)
        low = (gain_ref[...] - high.astype(f32)).astype(bf16)
        which = lax.broadcasted_iota(jnp.int32, (16, width), 0)
        pair = jnp.where(which == 0, high.astype(f32), jnp.where(which == 1, low.astype(f32), 0.0)).astype(bf16)

        def weigh(j, carry):
            cols = pl.ds(pl.multiple_of(j * block, block), block)
            both = jnp.dot(pair, w_v[:, cols], preferred_element_type=f32)
            u_v[:, cols] = jnp.broadcast_to(jnp.sum(both, axis=0, keepdims=True), (8, block))
            return carry

        lax.fori_loop(0, PIECES, weigh, 0)

    @pl.when(s == 0)
    def _():
        u_v[...] = jnp.zeros_like(u_v)

    @pl.when(jnp.logical_not(late))
    def _():
        for j in range(PIECES):
            w_copy(j).wait()
        prepare()

    pltpu.make_async_copy(stored_hbm.at[0, 1], keep_v, sem_keep).wait()

    def remote(src, dst, send, recv, device):
        return pltpu.make_async_remote_copy(
            src_ref=src, dst_ref=dst, send_sem=send, recv_sem=recv, device_id=device, device_id_type=MESH)

    def cols_of(j):
        return pl.ds(pl.multiple_of(j * block, block), block)

    def fcopy(c, cols):
        return remote(clip_v.at[c, :, cols], fin_v.at[c, :, cols], fsend.at[c], frecv.at[c], nxt)

    def fwhole(c):
        return remote(clip_v.at[c], fin_v.at[c], fsend.at[c], frecv.at[c], nxt)

    def bcopy(c, j):
        cols = cols_of(j)
        return remote(clip_v.at[c, :, cols], bin_v.at[c, :, cols], bsend.at[c, j], brecv.at[c, j], prv)

    def place(c):
        batch = c // per_batch
        first = pl.multiple_of((c % per_batch) * rows, rows)
        sample = ids_ref[0, batch]
        index = jnp.where(s == 0, batch, sample)
        return batch, first, sample, index

    share = width // 4
    part = share // 4
    unit = width // 12
    split = unit * Z_UNITS
    low_lanes = pl.ds(0, split)
    high_lanes = pl.ds(split, width - split)

    def chunk_rows(c, n=1):
        return pl.ds(pl.multiple_of(c * rows, rows), n * rows)

    circle = ((0, z_up, dev_up), (1, z_down, dev_down), (2, z_far, dev_far))

    def z_copy(c, slot):
        return remote(gown_v.at[chunk_rows(c), low_lanes],
                      gz_v.at[pl.ds(pl.multiple_of(slot * local + c * rows, rows), rows)],
                      zsend.at[slot, c], zrecv.at[slot, c], circle[slot][2])

    def g_copy(c):
        return remote(gown_v.at[chunk_rows(c), high_lanes], gy_v.at[chunk_rows(c)], gsend.at[c], grecv.at[c], dev_row)

    def ncopy(slot):
        return remote(nt_v.at[circle[slot][1]],
                      ngat_v.at[:, pl.ds((slot + 1) * local, local)], nsend.at[slot], nrecv.at[slot], circle[slot][2])

    def nrow_copy():
        return remote(nt_v.at[:, pl.ds(pl.multiple_of((1 - row) * 2 * part, 2 * part), 2 * part)], nrow_v,
                      nsend.at[3], nrecv.at[3], dev_row)

    def share_normed():
        step = share // 3
        def turn(i, carry):
            cols = pl.ds(pl.multiple_of(i * step, step), step)
            for b in range(batches):
                values = normed_v[pl.ds(b * per_batch, per_batch), :, cols].reshape(tokens, step)
                nt_v[i // 3, pl.ds(pl.multiple_of((i % 3) * step, step), step), pl.ds(b * tokens, tokens)] = values.T
            return carry
        lax.fori_loop(0, width // step, turn, 0)
        for slot in range(3):
            ncopy(slot).start()
        nrow_copy().start()
        ngat_v[:, pl.ds(0, local)] = nt_v[z]

    def several(ref, c, n, cols=None):
        if cols is None:
            return ref[pl.ds(c, n)].reshape(n * rows, ref.shape[-1])
        return ref[pl.ds(c, n), :, cols].reshape(n * rows, cols.size)

    def keep(ref, c, n, value, cols=None):
        if cols is None:
            ref[pl.ds(c, n)] = value.reshape(n, rows, value.shape[-1])
        else:
            ref[pl.ds(c, n), :, cols] = value.reshape(n, rows, cols.size)

    def state_of(c, n, cols=None):
        batch, first, sample, index = place(c)
        if cols is None:
            return base_v[index, pl.ds(first, n * rows), :].astype(f32) + several(fin_v, c, n).astype(f32)
        return base_v[index, pl.ds(first, n * rows), cols].astype(f32) + several(fin_v, c, n, cols).astype(f32)

    def forward(c, n, final):
        batch, first, sample, index = place(c)
        if final:
            for i in range(n):
                fwhole(c + i).wait_recv()
        else:
            @pl.when(has_prev)
            def _():
                fwhole(c).wait_recv()

        x = state_of(c, n)
        mu = jnp.mean(x, axis=-1, keepdims=True)
        xc = x - mu
        var = jnp.mean(xc * xc, axis=-1, keepdims=True)
        rs = lax.rsqrt(var + epsilon)
        keep(normed_v, c, n, (xc * rs * gain_ref[...]).astype(bf16))
        keep(mu_v, c, n, jnp.broadcast_to(mu, (n * rows, 128)))
        keep(rs_v, c, n, jnp.broadcast_to(rs, (n * rows, 128)))

        pieces = 2 * PIECES if final else PIECES
        narrow = width // pieces

        def tile(j, carry2):
            cols = pl.ds(pl.multiple_of(j * narrow, narrow), narrow)
            if not final:
                @pl.when(jnp.logical_and(c == 0, late))
                def _():
                    w_copy(j).wait()

            v = jnp.dot(several(normed_v, c, n), w_v[:, cols], preferred_element_type=f32)
            cdf = 0.5 + 0.5 * lax.erf(v * rsqrt2)
            res = state_of(c, n, cols) + v * cdf
            out_v[batch, pl.ds(first, n * rows), cols] = res.astype(bf16)
            if not final:
                kept = keep_v[sample, pl.ds(first, rows), cols].astype(f32)
                clip_v[c, :, cols] = jnp.clip(res - kept, -delta_bound, delta_bound).astype(bf16)
                fcopy(c, cols).start()
                keep(pre_v, c, n, v, cols)
            slope = cdf + v * (jnp.exp(-0.5 * v * v) * rsqrt2pi)
            if not final:
                keep(slope_v, c, n, slope.astype(bf16), cols)
                return carry2
            up = res * scale
            keep(pre_v, 0, n, up, cols)
            return push_back(c, n, cols, slope * up, v, carry2)

        zero = jnp.zeros((n * rows, 1), f32)
        sums = lax.fori_loop(0, pieces, tile, (zero, zero) if final else 0)
        return sums

    def push_back(c, n, cols, value, v, sums):
        gp = value.astype(bf16)
        gown_v[chunk_rows(c, n), cols] = gp
        wide_gp = gp.astype(f32)
        return (
            sums[0] + jnp.sum(wide_gp * u_v[0:1, cols], axis=-1, keepdims=True),
            sums[1] + jnp.sum(wide_gp * v, axis=-1, keepdims=True),
        )

    def backward(c, n, sums):
        final = sums is not None

        def piece(j, sums):
            cols = cols_of(j)
            bcopy(c, j).wait_recv()
            up = several(bin_v, c, n, cols).astype(f32)
            return push_back(c, n, cols, several(slope_v, c, n, cols).astype(f32) * up, several(pre_v, c, n, cols), sums)

        if not final:
            zero = jnp.zeros((n * rows, 1), f32)
            sums = lax.fori_loop(0, PIECES, piece, (zero, zero))
        for i in range(n):
            for slot in range(3):
                z_copy(c + i, slot).start()

        if not final:
            @pl.when(s == 0)
            def _():
                g_copy(c).start()

        def pull():
            m1 = sums[0] * (1.0 / width)
            m2 = sums[1] * (1.0 / width)
            mu = several(mu_v, c, n)[:, :1]
            rs = several(rs_v, c, n)[:, :1]
            if not final:
                fwhole(c).wait_send()

            def tile(j, carry2):
                cols = cols_of(j)
                gn = jnp.dot(gown_v[chunk_rows(c, n)], wt_v[:, cols], preferred_element_type=f32)
                state = state_of(c, n, cols)
                xhat = (state - mu) * rs
                if final:
                    up = several(pre_v, 0, n, cols)
                else:
                    up = several(bin_v, c, n, cols).astype(f32)
                sent = up + rs * (gn * gain_ref[:, cols] - m1 - xhat * m2)
                keep(clip_v, c, n, sent.astype(bf16), cols)
                bcopy(c, j).start()
                return carry2

            lax.fori_loop(0, PIECES, tile, 0)
            for i in range(1, n):
                for j in range(PIECES):
                    bcopy(c + i, j).start()

        if final:
            pull()
        else:
            pl.when(has_prev)(pull)

    def forward_step(c, carry):
        forward(c, 1, False)
        return carry

    def backward_step(c, carry):
        backward(c, 1, None)
        return carry

    def pair_step(t, carry):
        sums = forward(2 * t, 2, True)

        backward(2 * t, 2, sums)
        return carry

    @pl.when(has_next)
    def _():
        lax.fori_loop(0, chunks, forward_step, 0)

        @pl.when(late)
        def _():
            share_normed()

            @pl.when(has_prev)
            def _():
                prepare()

        lax.fori_loop(0, chunks, backward_step, 0)

    @pl.when(s == last)
    def _():
        lax.fori_loop(0, chunks // 2, pair_step, 0)

    for peer in (dev_up, dev_down, dev_far, dev_core, dev_row):
        pl.semaphore_signal(ready, inc=1, device_id=peer, device_id_type=MESH)

    def start_rows(c, carry):
        g_copy(c).start()
        return carry

    @pl.when(has_prev)
    def _():
        lax.fori_loop(0, chunks, start_rows, 0)

    @pl.when(jnp.logical_not(late))
    def _():
        share_normed()

    def band(place_of, lanes, count=1):
        return (pl.ds(place_of * part, count * part), lanes)

    def lanes_of(q):
        return pl.ds(pl.multiple_of(q * unit, unit), unit)

    def core_copy(q, y):
        lanes = lanes_of(q)
        return remote(w_v.at[band(y, lanes)], wt_v.at[band(y, lanes)], csend.at[q, y], crecv.at[q, y], dev_core)

    def row_copy(q):
        lanes = lanes_of(q)
        return remote(w_v.at[band(4, lanes)], wt_v.at[band(2, lanes)], ysend.at[q], yrecv.at[q], dev_row)

    def core_copy2(q):
        lanes = lanes_of(q)
        return remote(w_v.at[band(6, lanes, 4)], wt_v.at[band(3, lanes, 4)], csend2.at[q], crecv2.at[q], dev_core)

    def sum_rows(z_of):
        return pl.ds(pl.multiple_of((10 + z_of) * part, part), part)

    def far_half(q, side):
        lanes = lanes_of(q)
        lines = pl.ds(pl.multiple_of((10 + z_far) * part + side * (part // 2), part // 2), part // 2)
        return remote(w_v.at[lines, lanes], wt_v.at[pl.ds(7 * part + side * (part // 2), part // 2), lanes],
                      zsend2.at[side, q], zrecv2.at[side, q], circle[side][2])

    def near_block(q, side):
        lanes = lanes_of(q)
        return remote(w_v.at[sum_rows(circle[side][1]), lanes], wt_v.at[band(8 + side, lanes)],
                      zsend2.at[2 + side, q], zrecv2.at[2 + side, q], circle[side][2])

    def came(c, carry):
        g_copy(c).wait_recv()
        return carry

    pl.semaphore_wait(ready, 5)

    def high_product(whose, lanes, high):
        mine = nt_v[:, pl.ds(pl.multiple_of(row * 2 * part + whose * part, part), part)].reshape(share, local)
        theirs = nrow_v[:, pl.ds(pl.multiple_of(whose * part, part), part)].reshape(share, local)
        return (
            jnp.dot(mine, gown_v[:, lanes], preferred_element_type=f32)
            + jnp.dot(theirs, gy_v[:, high], preferred_element_type=f32)
        ).astype(bf16)

    def product2(q):
        lanes = lanes_of(q)
        high = pl.ds(pl.multiple_of((q - Z_UNITS) * unit, unit), unit)
        w_v[band(6, lanes, 4)] = high_product(1 - core, lanes, high)
        core_copy2(q).start()
        w_v[band(10, lanes, 4)] = high_product(core, lanes, high)

    def pair_sum2(q):
        lanes = lanes_of(q)
        core_copy2(q).wait_recv()
        w_v[band(10, lanes, 4)] = (
            w_v[band(10, lanes, 4)].astype(f32) + wt_v[band(3, lanes, 4)].astype(f32)
        ).astype(bf16)
        for side in range(2):
            far_half(q, side).start()

    def near_sum2(q):
        lanes = lanes_of(q)
        for side in range(2):
            far_half(q, side).wait_recv()
            lines = pl.ds(pl.multiple_of((10 + circle[side][1]) * part + side * (part // 2), part // 2), part // 2)
            w_v[lines, lanes] = (
                w_v[lines, lanes].astype(f32)
                + wt_v[pl.ds(7 * part + side * (part // 2), part // 2), lanes].astype(f32)
            ).astype(bf16)
            near_block(q, side).start()

    def arrived(c, carry):
        for slot in range(3):
            z_copy(c, slot).wait_recv()
        return carry

    def low_product(y, whose, lanes):
        lines = pl.ds(pl.multiple_of(y * 2 * part + whose * part, part), part)
        return (
            jnp.dot(ngat_v[lines, pl.ds(0, local)], gown_v[:, lanes], preferred_element_type=f32)
            + jnp.dot(ngat_v[lines, pl.ds(local, 3 * local)], gz_v[:, lanes], preferred_element_type=f32)
        ).astype(bf16)

    def one_of(first, which):
        return pl.ds(pl.multiple_of((first + which) * part, part), part)

    def product(q):
        lanes = lanes_of(q)
        for y in range(2):
            w_v[band(y, lanes)] = low_product(y, 1 - core, lanes)
            core_copy(q, y).start()
        for y in range(2):
            w_v[band(2 + y, lanes)] = low_product(y, core, lanes)

    def pair_sum(q):
        lanes = lanes_of(q)
        for y in range(2):
            core_copy(q, y).wait_recv()
        w_v[band(4, lanes)] = (
            w_v[one_of(2, 1 - row), lanes].astype(f32) + wt_v[one_of(0, 1 - row), lanes].astype(f32)
        ).astype(bf16)
        row_copy(q).start()

    high_units = 12 - Z_UNITS
    high_first = jnp.where(s == 0, 0, Z_UNITS)
    low_first = jnp.where(s == 0, high_units, 0)
    near_lag = jnp.where(s == 0, NEAR_LAG, 2)

    def tail(t, carry):
        def at(begin, count, work, shift):
            @pl.when(jnp.logical_and(t >= begin, t < begin + count))
            def _():
                work(t - begin + shift)

        @pl.when(t == high_first)
        def _():
            nrow_copy().wait_recv()
            lax.fori_loop(0, chunks, came, 0)

        at(high_first, high_units, product2, Z_UNITS)
        at(high_first + LAG, high_units, pair_sum2, Z_UNITS)

        @pl.when(t == low_first)
        def _():
            for slot in range(3):
                ncopy(slot).wait_recv()
            lax.fori_loop(0, chunks, arrived, 0)

        at(low_first, Z_UNITS, product, 0)
        at(low_first + LAG, Z_UNITS, pair_sum, 0)
        at(high_first + LAG + near_lag, high_units, near_sum2, Z_UNITS)
        return carry

    lax.fori_loop(0, jnp.where(s == 0, max(12 + LAG, LAG + NEAR_LAG + high_units), 12 + LAG + 2), tail, 0)

    def total2(q, carry):
        lanes = lanes_of(q)
        result = w_v[sum_rows(z), lanes].astype(f32)
        for side in range(2):
            near_block(q, side).wait_recv()
            result += wt_v[band(8 + side, lanes)].astype(f32)
        wgrad_v[:, lanes] = result.astype(bf16)
        return carry

    def total(q, carry):
        lanes = lanes_of(q)
        row_copy(q).wait_recv()
        wgrad_v[:, lanes] = (
            w_v[one_of(2, row), lanes].astype(f32) + wt_v[one_of(0, row), lanes].astype(f32)
            + wt_v[band(2, lanes)].astype(f32)
        ).astype(bf16)
        return carry

    def totals(t, carry):
        q = (t + jnp.where(s == 0, Z_UNITS, 0)) % 12

        @pl.when(q < Z_UNITS)
        def _():
            total(q, 0)

        @pl.when(q >= Z_UNITS)
        def _():
            total2(q, 0)

        return carry

    lax.fori_loop(0, 12, totals, 0)

    def finish(c, carry):
        g_copy(c).wait_send()
        for slot in range(3):
            z_copy(c, slot).wait_send()

        @pl.when(s == 0)
        def _():
            fwhole(c).wait_send()

        @pl.when(has_prev)
        def _():
            for j in range(PIECES):
                bcopy(c, j).wait_send()

        return carry

    lax.fori_loop(0, chunks, finish, 0)

    def finish_low(q, carry):
        for y in range(2):
            core_copy(q, y).wait_send()
        row_copy(q).wait_send()
        return carry

    def finish_high(q, carry):
        core_copy2(q).wait_send()
        for side in range(2):
            far_half(q, side).wait_send()
            near_block(q, side).wait_send()
        return carry

    lax.fori_loop(0, Z_UNITS, finish_low, 0)
    lax.fori_loop(Z_UNITS, 12, finish_high, 0)
    for slot in range(3):
        ncopy(slot).wait_send()
    nrow_copy().wait_send()


def relay(scale, inputs, sample_ids, stored, weight, norm_gain):
    batches, tokens, width = inputs.shape
    rows = min(CHUNK, tokens)
    local = batches * tokens
    chunks = local // rows
    share = width // 4
    part = share // 4
    split = width // 12 * Z_UNITS
    any_spec = pl.BlockSpec(memory_space=pl.ANY)
    chunked = pltpu.VMEM((chunks, rows, width), bf16)
    dma = pltpu.SemaphoreType.DMA
    return pl.pallas_call(
        functools.partial(relay_kernel, scale),
        out_shape=(
            pltpu.VMEM(inputs.shape, bf16),
            pltpu.VMEM((part, width), bf16),
        ),
        in_specs=[
            pl.BlockSpec(memory_space=pltpu.SMEM), any_spec, any_spec, any_spec,
            pl.BlockSpec(memory_space=pltpu.VMEM),
        ],
        out_specs=(pl.BlockSpec(memory_space=pltpu.VMEM), pl.BlockSpec(memory_space=pltpu.VMEM)),
        scratch_shapes=[
            pltpu.VMEM((width, width), bf16),
            pltpu.VMEM((width, width), bf16),
            pltpu.VMEM(inputs.shape, bf16),
            pltpu.VMEM(inputs.shape, bf16),
            chunked, chunked, chunked,
            pltpu.VMEM((chunks, rows, width), f32),
            chunked, chunked,
            pltpu.VMEM((chunks, rows, 128), f32),
            pltpu.VMEM((chunks, rows, 128), f32),
            pltpu.VMEM((8, width), f32),
            pltpu.VMEM((4, share, local), bf16),
            pltpu.VMEM((share, 4 * local), bf16),
            pltpu.VMEM((4, 2 * part, local), bf16),
            pltpu.VMEM((local, width), bf16),
            pltpu.VMEM((3 * local, split), bf16),
            pltpu.VMEM((local, width - split), bf16),
            dma((PIECES,)), dma, dma,
            dma((chunks,)), dma((chunks,)),
            dma((chunks, PIECES)), dma((chunks, PIECES)),
            dma((4,)), dma((4,)),
            dma((3, chunks)), dma((3, chunks)),
            dma((chunks,)), dma((chunks,)),
            dma((Z_UNITS, 2)), dma((Z_UNITS, 2)),
            dma((Z_UNITS,)), dma((Z_UNITS,)),
            dma((12,)), dma((12,)),
            dma((4, 12)), dma((4, 12)),
            pltpu.SemaphoreType.REGULAR,
        ],
        compiler_params=pltpu.CompilerParams(
            collective_id=0, has_side_effects=True, vmem_limit_bytes=VMEM_LIMIT),
        cost_estimate=pl.CostEstimate(
            flops=6 * local * width * width, bytes_accessed=2 * width * width, transcendentals=0),
        name="relay",
    )(sample_ids, inputs, stored, weight, norm_gain)


def per_device(inputs, sample_ids, stored, weight, norm_gain):
    batches, tokens, width = inputs.shape
    scale = 1.0 / math.sqrt(lax.axis_size("dp") * batches * tokens)
    outs, summed = relay(scale, inputs, sample_ids, stored, weight, norm_gain)
    return (outs[None], summed[None])


def solution(mesh):
    return jax.shard_map(
        per_device,
        mesh=mesh,
        in_specs=(
            P("dp", None, None),
            P("dp", None),
            P("section", None, "dp", None, None),
            P("section", None, None),
            P("section", None),
        ),
        out_specs=(P("section", "dp", None, None), P("section", "dp", None)),
        check_vma=False,
    )
```

```python
import functools
import math

import jax
import jax.numpy as jnp
from jax import lax
from jax.experimental import pallas as pl
from jax.experimental.pallas import tpu as pltpu
from jax.sharding import PartitionSpec as P

epsilon = 1e-05
delta_bound = 2.0
CHUNK = 32
PIECES = 4
Z_UNITS = 7
VMEM_LIMIT = 64200000
FIRST_COLUMNS = 2
LAG = 2
NEAR_LAG = 6
MESH = pl.DeviceIdType.MESH
f32 = jnp.float32
bf16 = jnp.bfloat16
rsqrt2 = 1.0 / math.sqrt(2.0)
rsqrt2pi = 1.0 / math.sqrt(2.0 * math.pi)


def relay_kernel(
    scale,
    ids_ref, inputs_hbm, stored_hbm, w_hbm, gain_ref,
    out_v, wgrad_v,
    w_v, wt_v, base_v, keep_v, fin_v, clip_v, normed_v, pre_v, slope_v, bin_v,
    mu_v, rs_v, u_v,
    nt_v, ngat_v, nrow_v, gown_v, gz_v, gy_v,
    sem_w, sem_base, sem_keep, fsend, frecv, bsend, brecv,
    nsend, nrecv, zsend, zrecv, gsend, grecv, csend, crecv, ysend, yrecv,
    csend2, crecv2, zsend2, zrecv2, ready,
):
    s = lax.axis_index("section")
    sections = lax.axis_size("section")
    d = lax.axis_index("dp")
    last = sections - 1
    chunks, rows, width = fin_v.shape
    tokens = base_v.shape[1]
    batches = base_v.shape[0]
    local = chunks * rows
    per_batch = tokens // rows
    block = width // PIECES
    has_next = s < last
    has_prev = s > 0
    nxt = {"section": jnp.minimum(s + 1, last)}
    prv = {"section": jnp.maximum(s - 1, 0)}
    z = d // 4
    rest = d % 4
    core = d % 2
    row = rest // 2
    z_up = (z + 1) % 4
    z_down = (z + 3) % 4
    z_far = (z + 2) % 4
    dev_up = {"dp": z_up * 4 + rest}
    dev_down = {"dp": z_down * 4 + rest}
    dev_far = {"dp": z_far * 4 + rest}
    dev_core = {"dp": d + 1 - 2 * core}
    dev_row = {"dp": z * 4 + (rest + 2) % 4}

    late = s < last - 2

    def w_copy(j):
        cols = pl.ds(pl.multiple_of(j * block, block), block)
        return pltpu.make_async_copy(w_hbm.at[0, :, cols], w_v.at[:, cols], sem_w.at[j])

    @pl.when(s == 0)
    def _():
        pltpu.make_async_copy(inputs_hbm, base_v, sem_base).start()

    @pl.when(has_prev)
    def _():
        pltpu.make_async_copy(stored_hbm.at[0, 0], base_v, sem_base).start()

    pltpu.make_async_copy(stored_hbm.at[0, 1], keep_v, sem_keep).start()
    for j in range(FIRST_COLUMNS):
        w_copy(j).start()

    barrier = pltpu.get_barrier_semaphore()

    @pl.when(has_next)
    def _():
        pl.semaphore_signal(barrier, inc=1, device_id=nxt, device_id_type=MESH)

    @pl.when(has_prev)
    def _():
        pl.semaphore_signal(barrier, inc=1, device_id=prv, device_id_type=MESH)

    for peer in (dev_up, dev_down, dev_far, dev_core, dev_row):
        pl.semaphore_signal(barrier, inc=1, device_id=peer, device_id_type=MESH)
    pl.semaphore_wait(barrier, 5 + jnp.minimum(s, 1) + jnp.minimum(last - s, 1))

    @pl.when(s == 0)
    def _():
        fin_v[...] = jnp.zeros_like(fin_v)

    pltpu.make_async_copy(inputs_hbm, base_v, sem_base).wait()
    for j in range(FIRST_COLUMNS, PIECES):
        w_copy(j).start()
    def prepare():
        side = 256
        line = lax.broadcasted_iota(jnp.int32, (side, side), 0)
        column = lax.broadcasted_iota(jnp.int32, (side, side), 1)
        eye = jnp.where(line == column, 1.0, 0.0).astype(bf16)

        def turn(i, carry):
            cols = pl.ds(pl.multiple_of(i * side, side), side)
            for j in range(PIECES):
                part = pl.ds(j * block, block)
                wt_v[cols, part] = lax.dot_general(
                    eye, w_v[part, cols], (((1,), (1,)), ((), ())), preferred_element_type=f32).astype(bf16)
            return carry

        lax.fori_loop(0, width // side, turn, 0)
        high = gain_ref[...].astype(bf16)
        low = (gain_ref[...] - high.astype(f32)).astype(bf16)
        which = lax.broadcasted_iota(jnp.int32, (16, width), 0)
        pair = jnp.where(which == 0, high.astype(f32), jnp.where(which == 1, low.astype(f32), 0.0)).astype(bf16)

        def weigh(j, carry):
            cols = pl.ds(pl.multiple_of(j * block, block), block)
            both = jnp.dot(pair, w_v[:, cols], preferred_element_type=f32)
            u_v[:, cols] = jnp.broadcast_to(jnp.sum(both, axis=0, keepdims=True), (8, block))
            return carry

        lax.fori_loop(0, PIECES, weigh, 0)

    @pl.when(s == 0)
    def _():
        u_v[...] = jnp.zeros_like(u_v)

    @pl.when(jnp.logical_not(late))
    def _():
        for j in range(PIECES):
            w_copy(j).wait()
        prepare()

    pltpu.make_async_copy(stored_hbm.at[0, 1], keep_v, sem_keep).wait()

    def remote(src, dst, send, recv, device):
        return pltpu.make_async_remote_copy(
            src_ref=src, dst_ref=dst, send_sem=send, recv_sem=recv, device_id=device, device_id_type=MESH)

    def cols_of(j):
        return pl.ds(pl.multiple_of(j * block, block), block)

    def fcopy(c, cols):
        return remote(clip_v.at[c, :, cols], fin_v.at[c, :, cols], fsend.at[c], frecv.at[c], nxt)

    def fwhole(c):
        return remote(clip_v.at[c], fin_v.at[c], fsend.at[c], frecv.at[c], nxt)

    def bcopy(c, j):
        cols = cols_of(j)
        return remote(clip_v.at[c, :, cols], bin_v.at[c, :, cols], bsend.at[c, j], brecv.at[c, j], prv)

    def place(c):
        batch = c // per_batch
        first = pl.multiple_of((c % per_batch) * rows, rows)
        sample = ids_ref[0, batch]
        index = jnp.where(s == 0, batch, sample)
        return batch, first, sample, index

    share = width // 4
    part = share // 4
    unit = width // 12
    split = unit * Z_UNITS
    low_lanes = pl.ds(0, split)
    high_lanes = pl.ds(split, width - split)

    def chunk_rows(c, n=1):
        return pl.ds(pl.multiple_of(c * rows, rows), n * rows)

    circle = ((0, z_up, dev_up), (1, z_down, dev_down), (2, z_far, dev_far))

    def z_copy(c, slot):
        return remote(gown_v.at[chunk_rows(c), low_lanes],
                      gz_v.at[pl.ds(pl.multiple_of(slot * local + c * rows, rows), rows)],
                      zsend.at[slot, c], zrecv.at[slot, c], circle[slot][2])

    def g_copy(c):
        return remote(gown_v.at[chunk_rows(c), high_lanes], gy_v.at[chunk_rows(c)], gsend.at[c], grecv.at[c], dev_row)

    def ncopy(slot):
        return remote(nt_v.at[circle[slot][1]],
                      ngat_v.at[:, pl.ds((slot + 1) * local, local)], nsend.at[slot], nrecv.at[slot], circle[slot][2])

    def nrow_copy():
        return remote(nt_v.at[:, pl.ds(pl.multiple_of((1 - row) * 2 * part, 2 * part), 2 * part)], nrow_v,
                      nsend.at[3], nrecv.at[3], dev_row)

    def share_normed():
        step = share // 3
        def turn(i, carry):
            cols = pl.ds(pl.multiple_of(i * step, step), step)
            for b in range(batches):
                values = normed_v[pl.ds(b * per_batch, per_batch), :, cols].reshape(tokens, step)
                nt_v[i // 3, pl.ds(pl.multiple_of((i % 3) * step, step), step), pl.ds(b * tokens, tokens)] = values.T
            return carry
        lax.fori_loop(0, width // step, turn, 0)
        for slot in range(3):
            ncopy(slot).start()
        nrow_copy().start()
        ngat_v[:, pl.ds(0, local)] = nt_v[z]

    def several(ref, c, n, cols=None):
        if cols is None:
            return ref[pl.ds(c, n)].reshape(n * rows, ref.shape[-1])
        return ref[pl.ds(c, n), :, cols].reshape(n * rows, cols.size)

    def keep(ref, c, n, value, cols=None):
        if cols is None:
            ref[pl.ds(c, n)] = value.reshape(n, rows, value.shape[-1])
        else:
            ref[pl.ds(c, n), :, cols] = value.reshape(n, rows, cols.size)

    def state_of(c, n, cols=None):
        batch, first, sample, index = place(c)
        if cols is None:
            return base_v[index, pl.ds(first, n * rows), :].astype(f32) + several(fin_v, c, n).astype(f32)
        return base_v[index, pl.ds(first, n * rows), cols].astype(f32) + several(fin_v, c, n, cols).astype(f32)

    def forward(c, n, final):
        batch, first, sample, index = place(c)
        if final:
            for i in range(n):
                fwhole(c + i).wait_recv()
        else:
            @pl.when(has_prev)
            def _():
                fwhole(c).wait_recv()

        x = state_of(c, n)
        mu = jnp.mean(x, axis=-1, keepdims=True)
        xc = x - mu
        var = jnp.mean(xc * xc, axis=-1, keepdims=True)
        rs = lax.rsqrt(var + epsilon)
        keep(normed_v, c, n, (xc * rs * gain_ref[...]).astype(bf16))
        keep(mu_v, c, n, jnp.broadcast_to(mu, (n * rows, 128)))
        keep(rs_v, c, n, jnp.broadcast_to(rs, (n * rows, 128)))

        pieces = 2 * PIECES if final else PIECES
        narrow = width // pieces

        def tile(j, carry2):
            cols = pl.ds(pl.multiple_of(j * narrow, narrow), narrow)
            if not final:
                @pl.when(jnp.logical_and(c == 0, late))
                def _():
                    w_copy(j).wait()

            v = jnp.dot(several(normed_v, c, n), w_v[:, cols], preferred_element_type=f32)
            cdf = 0.5 + 0.5 * lax.erf(v * rsqrt2)
            res = state_of(c, n, cols) + v * cdf
            out_v[batch, pl.ds(first, n * rows), cols] = res.astype(bf16)
            if not final:
                kept = keep_v[sample, pl.ds(first, rows), cols].astype(f32)
                clip_v[c, :, cols] = jnp.clip(res - kept, -delta_bound, delta_bound).astype(bf16)
                fcopy(c, cols).start()
                keep(pre_v, c, n, v, cols)
            slope = cdf + v * (jnp.exp(-0.5 * v * v) * rsqrt2pi)
            if not final:
                keep(slope_v, c, n, slope.astype(bf16), cols)
                return carry2
            up = res * scale
            keep(pre_v, 0, n, up, cols)
            return push_back(c, n, cols, slope * up, v, carry2)

        zero = jnp.zeros((n * rows, 1), f32)
        sums = lax.fori_loop(0, pieces, tile, (zero, zero) if final else 0)
        return sums

    def push_back(c, n, cols, value, v, sums):
        gp = value.astype(bf16)
        gown_v[chunk_rows(c, n), cols] = gp
        wide_gp = gp.astype(f32)
        return (
            sums[0] + jnp.sum(wide_gp * u_v[0:1, cols], axis=-1, keepdims=True),
            sums[1] + jnp.sum(wide_gp * v, axis=-1, keepdims=True),
        )

    def backward(c, n, sums):
        final = sums is not None

        def piece(j, sums):
            cols = cols_of(j)
            bcopy(c, j).wait_recv()
            up = several(bin_v, c, n, cols).astype(f32)
            return push_back(c, n, cols, several(slope_v, c, n, cols).astype(f32) * up, several(pre_v, c, n, cols), sums)

        if not final:
            zero = jnp.zeros((n * rows, 1), f32)
            sums = lax.fori_loop(0, PIECES, piece, (zero, zero))
        for i in range(n):
            for slot in range(3):
                z_copy(c + i, slot).start()

        if not final:
            @pl.when(s == 0)
            def _():
                g_copy(c).start()

        def pull():
            m1 = sums[0] * (1.0 / width)
            m2 = sums[1] * (1.0 / width)
            mu = several(mu_v, c, n)[:, :1]
            rs = several(rs_v, c, n)[:, :1]
            if not final:
                fwhole(c).wait_send()

            def tile(j, carry2):
                cols = cols_of(j)
                gn = jnp.dot(gown_v[chunk_rows(c, n)], wt_v[:, cols], preferred_element_type=f32)
                state = state_of(c, n, cols)
                xhat = (state - mu) * rs
                if final:
                    up = several(pre_v, 0, n, cols)
                else:
                    up = several(bin_v, c, n, cols).astype(f32)
                sent = up + rs * (gn * gain_ref[:, cols] - m1 - xhat * m2)
                keep(clip_v, c, n, sent.astype(bf16), cols)
                bcopy(c, j).start()
                return carry2

            lax.fori_loop(0, PIECES, tile, 0)
            for i in range(1, n):
                for j in range(PIECES):
                    bcopy(c + i, j).start()

        if final:
            pull()
        else:
            pl.when(has_prev)(pull)

    def forward_step(c, carry):
        forward(c, 1, False)
        return carry

    def backward_step(c, carry):
        backward(c, 1, None)
        return carry

    def pair_step(t, carry):
        sums = forward(2 * t, 2, True)

        backward(2 * t, 2, sums)
        return carry

    @pl.when(has_next)
    def _():
        lax.fori_loop(0, chunks, forward_step, 0)

        @pl.when(late)
        def _():
            share_normed()

            @pl.when(has_prev)
            def _():
                prepare()

        lax.fori_loop(0, chunks, backward_step, 0)

    @pl.when(s == last)
    def _():
        lax.fori_loop(0, chunks // 2, pair_step, 0)

    for peer in (dev_up, dev_down, dev_far, dev_core, dev_row):
        pl.semaphore_signal(ready, inc=1, device_id=peer, device_id_type=MESH)

    def start_rows(c, carry):
        g_copy(c).start()
        return carry

    @pl.when(has_prev)
    def _():
        lax.fori_loop(0, chunks, start_rows, 0)

    @pl.when(jnp.logical_not(late))
    def _():
        share_normed()

    def band(place_of, lanes, count=1):
        return (pl.ds(place_of * part, count * part), lanes)

    def lanes_of(q):
        return pl.ds(pl.multiple_of(q * unit, unit), unit)

    def core_copy(q, y):
        lanes = lanes_of(q)
        return remote(w_v.at[band(y, lanes)], wt_v.at[band(y, lanes)], csend.at[q, y], crecv.at[q, y], dev_core)

    def row_copy(q):
        lanes = lanes_of(q)
        return remote(w_v.at[band(4, lanes)], wt_v.at[band(2, lanes)], ysend.at[q], yrecv.at[q], dev_row)

    def core_copy2(q):
        lanes = lanes_of(q)
        return remote(w_v.at[band(6, lanes, 4)], wt_v.at[band(3, lanes, 4)], csend2.at[q], crecv2.at[q], dev_core)

    def sum_rows(z_of):
        return pl.ds(pl.multiple_of((10 + z_of) * part, part), part)

    def far_half(q, side):
        lanes = lanes_of(q)
        lines = pl.ds(pl.multiple_of((10 + z_far) * part + side * (part // 2), part // 2), part // 2)
        return remote(w_v.at[lines, lanes], wt_v.at[pl.ds(7 * part + side * (part // 2), part // 2), lanes],
                      zsend2.at[side, q], zrecv2.at[side, q], circle[side][2])

    def near_block(q, side):
        lanes = lanes_of(q)
        return remote(w_v.at[sum_rows(circle[side][1]), lanes], wt_v.at[band(8 + side, lanes)],
                      zsend2.at[2 + side, q], zrecv2.at[2 + side, q], circle[side][2])

    def came(c, carry):
        g_copy(c).wait_recv()
        return carry

    pl.semaphore_wait(ready, 5)

    def high_product(whose, lanes, high):
        mine = nt_v[:, pl.ds(pl.multiple_of(row * 2 * part + whose * part, part), part)].reshape(share, local)
        theirs = nrow_v[:, pl.ds(pl.multiple_of(whose * part, part), part)].reshape(share, local)
        return (
            jnp.dot(mine, gown_v[:, lanes], preferred_element_type=f32)
            + jnp.dot(theirs, gy_v[:, high], preferred_element_type=f32)
        ).astype(bf16)

    def product2(q):
        lanes = lanes_of(q)
        high = pl.ds(pl.multiple_of((q - Z_UNITS) * unit, unit), unit)
        w_v[band(6, lanes, 4)] = high_product(1 - core, lanes, high)
        core_copy2(q).start()
        w_v[band(10, lanes, 4)] = high_product(core, lanes, high)

    def pair_sum2(q):
        lanes = lanes_of(q)
        core_copy2(q).wait_recv()
        w_v[band(10, lanes, 4)] = (
            w_v[band(10, lanes, 4)].astype(f32) + wt_v[band(3, lanes, 4)].astype(f32)
        ).astype(bf16)
        for side in range(2):
            far_half(q, side).start()

    def near_sum2(q):
        lanes = lanes_of(q)
        for side in range(2):
            far_half(q, side).wait_recv()
            lines = pl.ds(pl.multiple_of((10 + circle[side][1]) * part + side * (part // 2), part // 2), part // 2)
            w_v[lines, lanes] = (
                w_v[lines, lanes].astype(f32)
                + wt_v[pl.ds(7 * part + side * (part // 2), part // 2), lanes].astype(f32)
            ).astype(bf16)
            near_block(q, side).start()

    def arrived(c, carry):
        for slot in range(3):
            z_copy(c, slot).wait_recv()
        return carry

    def low_product(y, whose, lanes):
        lines = pl.ds(pl.multiple_of(y * 2 * part + whose * part, part), part)
        return (
            jnp.dot(ngat_v[lines, pl.ds(0, local)], gown_v[:, lanes], preferred_element_type=f32)
            + jnp.dot(ngat_v[lines, pl.ds(local, 3 * local)], gz_v[:, lanes], preferred_element_type=f32)
        ).astype(bf16)

    def one_of(first, which):
        return pl.ds(pl.multiple_of((first + which) * part, part), part)

    def product(q):
        lanes = lanes_of(q)
        for y in range(2):
            w_v[band(y, lanes)] = low_product(y, 1 - core, lanes)
            core_copy(q, y).start()
        for y in range(2):
            w_v[band(2 + y, lanes)] = low_product(y, core, lanes)

    def pair_sum(q):
        lanes = lanes_of(q)
        for y in range(2):
            core_copy(q, y).wait_recv()
        w_v[band(4, lanes)] = (
            w_v[one_of(2, 1 - row), lanes].astype(f32) + wt_v[one_of(0, 1 - row), lanes].astype(f32)
        ).astype(bf16)
        row_copy(q).start()

    high_units = 12 - Z_UNITS
    high_first = jnp.where(s == 0, 0, Z_UNITS)
    low_first = jnp.where(s == 0, high_units, 0)
    near_lag = jnp.where(s == 0, NEAR_LAG, 2)

    def tail(t, carry):
        def at(begin, count, work, shift):
            @pl.when(jnp.logical_and(t >= begin, t < begin + count))
            def _():
                work(t - begin + shift)

        @pl.when(t == high_first)
        def _():
            nrow_copy().wait_recv()
            lax.fori_loop(0, chunks, came, 0)

        at(high_first, high_units, product2, Z_UNITS)
        at(high_first + LAG, high_units, pair_sum2, Z_UNITS)

        @pl.when(t == low_first)
        def _():
            for slot in range(3):
                ncopy(slot).wait_recv()
            lax.fori_loop(0, chunks, arrived, 0)

        at(low_first, Z_UNITS, product, 0)
        at(low_first + LAG, Z_UNITS, pair_sum, 0)
        at(high_first + LAG + near_lag, high_units, near_sum2, Z_UNITS)
        return carry

    lax.fori_loop(0, jnp.where(s == 0, max(12 + LAG, LAG + NEAR_LAG + high_units), 12 + LAG + 2), tail, 0)

    def total2(q, carry):
        lanes = lanes_of(q)
        result = w_v[sum_rows(z), lanes].astype(f32)
        for side in range(2):
            near_block(q, side).wait_recv()
            result += wt_v[band(8 + side, lanes)].astype(f32)
        wgrad_v[:, lanes] = result.astype(bf16)
        return carry

    def total(q, carry):
        lanes = lanes_of(q)
        row_copy(q).wait_recv()
        wgrad_v[:, lanes] = (
            w_v[one_of(2, row), lanes].astype(f32) + wt_v[one_of(0, row), lanes].astype(f32)
            + wt_v[band(2, lanes)].astype(f32)
        ).astype(bf16)
        return carry

    def totals(t, carry):
        q = (t + jnp.where(s == 0, Z_UNITS, 0)) % 12

        @pl.when(q < Z_UNITS)
        def _():
            total(q, 0)

        @pl.when(q >= Z_UNITS)
        def _():
            total2(q, 0)

        return carry

    lax.fori_loop(0, 12, totals, 0)

    def finish(c, carry):
        g_copy(c).wait_send()
        for slot in range(3):
            z_copy(c, slot).wait_send()

        @pl.when(s == 0)
        def _():
            fwhole(c).wait_send()

        @pl.when(has_prev)
        def _():
            for j in range(PIECES):
                bcopy(c, j).wait_send()

        return carry

    lax.fori_loop(0, chunks, finish, 0)

    def finish_low(q, carry):
        for y in range(2):
            core_copy(q, y).wait_send()
        row_copy(q).wait_send()
        return carry

    def finish_high(q, carry):
        core_copy2(q).wait_send()
        for side in range(2):
            far_half(q, side).wait_send()
            near_block(q, side).wait_send()
        return carry

    lax.fori_loop(0, Z_UNITS, finish_low, 0)
    lax.fori_loop(Z_UNITS, 12, finish_high, 0)
    for slot in range(3):
        ncopy(slot).wait_send()
    nrow_copy().wait_send()


def relay(scale, inputs, sample_ids, stored, weight, norm_gain):
    batches, tokens, width = inputs.shape
    rows = min(CHUNK, tokens)
    local = batches * tokens
    chunks = local // rows
    share = width // 4
    part = share // 4
    split = width // 12 * Z_UNITS
    any_spec = pl.BlockSpec(memory_space=pl.ANY)
    chunked = pltpu.VMEM((chunks, rows, width), bf16)
    dma = pltpu.SemaphoreType.DMA
    return pl.pallas_call(
        functools.partial(relay_kernel, scale),
        out_shape=(
            pltpu.VMEM(inputs.shape, bf16),
            pltpu.VMEM((part, width), bf16),
        ),
        in_specs=[
            pl.BlockSpec(memory_space=pltpu.SMEM), any_spec, any_spec, any_spec,
            pl.BlockSpec(memory_space=pltpu.VMEM),
        ],
        out_specs=(pl.BlockSpec(memory_space=pltpu.VMEM), pl.BlockSpec(memory_space=pltpu.VMEM)),
        scratch_shapes=[
            pltpu.VMEM((width, width), bf16),
            pltpu.VMEM((width, width), bf16),
            pltpu.VMEM(inputs.shape, bf16),
            pltpu.VMEM(inputs.shape, bf16),
            chunked, chunked, chunked,
            pltpu.VMEM((chunks, rows, width), f32),
            chunked, chunked,
            pltpu.VMEM((chunks, rows, 128), f32),
            pltpu.VMEM((chunks, rows, 128), f32),
            pltpu.VMEM((8, width), f32),
            pltpu.VMEM((4, share, local), bf16),
            pltpu.VMEM((share, 4 * local), bf16),
            pltpu.VMEM((4, 2 * part, local), bf16),
            pltpu.VMEM((local, width), bf16),
            pltpu.VMEM((3 * local, split), bf16),
            pltpu.VMEM((local, width - split), bf16),
            dma((PIECES,)), dma, dma,
            dma((chunks,)), dma((chunks,)),
            dma((chunks, PIECES)), dma((chunks, PIECES)),
            dma((4,)), dma((4,)),
            dma((3, chunks)), dma((3, chunks)),
            dma((chunks,)), dma((chunks,)),
            dma((Z_UNITS, 2)), dma((Z_UNITS, 2)),
            dma((Z_UNITS,)), dma((Z_UNITS,)),
            dma((12,)), dma((12,)),
            dma((4, 12)), dma((4, 12)),
            pltpu.SemaphoreType.REGULAR,
        ],
        compiler_params=pltpu.CompilerParams(
            collective_id=0, has_side_effects=True, vmem_limit_bytes=VMEM_LIMIT),
        cost_estimate=pl.CostEstimate(
            flops=6 * local * width * width, bytes_accessed=2 * width * width, transcendentals=0),
        name="relay",
    )(sample_ids, inputs, stored, weight, norm_gain)


def per_device(inputs, sample_ids, stored, weight, norm_gain):
    batches, tokens, width = inputs.shape
    scale = 1.0 / math.sqrt(lax.axis_size("dp") * batches * tokens)
    outs, summed = relay(scale, inputs, sample_ids, stored, weight, norm_gain)
    return (outs[None], summed[None])


def solution(mesh):
    return jax.shard_map(
        per_device,
        mesh=mesh,
        in_specs=(
            P("dp", None, None),
            P("dp", None),
            P("section", None, "dp", None, None),
            P("section", None, None),
            P("section", None),
        ),
        out_specs=(P("section", "dp", None, None), P("section", "dp", None)),
        check_vma=False,
    )
```

```python
import functools
import math

import jax
import jax.numpy as jnp
from jax import lax
from jax.experimental import pallas as pl
from jax.experimental.pallas import tpu as pltpu
from jax.sharding import PartitionSpec as P

epsilon = 1e-05
delta_bound = 2.0
CHUNK = 32
PIECES = 4
FINAL_PIECES = 6
Z_UNITS = 7
VMEM_LIMIT = 64200000
FIRST_COLUMNS = 2
LAG = 2
NEAR_LAG = 6
MESH = pl.DeviceIdType.MESH
f32 = jnp.float32
bf16 = jnp.bfloat16
rsqrt2 = 1.0 / math.sqrt(2.0)
rsqrt2pi = 1.0 / math.sqrt(2.0 * math.pi)


def relay_kernel(
    scale,
    ids_ref, inputs_hbm, stored_hbm, w_hbm, gain_ref,
    out_v, wgrad_v,
    w_v, wt_v, base_v, keep_v, fin_v, clip_v, normed_v, pre_v, slope_v, bin_v,
    mu_v, rs_v, u_v,
    nt_v, ngat_v, nrow_v, gown_v, gz_v, gy_v,
    sem_w, sem_base, sem_keep, fsend, frecv, bsend, brecv,
    nsend, nrecv, zsend, zrecv, gsend, grecv, csend, crecv, ysend, yrecv,
    csend2, crecv2, zsend2, zrecv2, ready,
):
    s = lax.axis_index("section")
    sections = lax.axis_size("section")
    d = lax.axis_index("dp")
    last = sections - 1
    chunks, rows, width = fin_v.shape
    tokens = base_v.shape[1]
    batches = base_v.shape[0]
    local = chunks * rows
    per_batch = tokens // rows
    block = width // PIECES
    has_next = s < last
    has_prev = s > 0
    nxt = {"section": jnp.minimum(s + 1, last)}
    prv = {"section": jnp.maximum(s - 1, 0)}
    z = d // 4
    rest = d % 4
    core = d % 2
    row = rest // 2
    z_up = (z + 1) % 4
    z_down = (z + 3) % 4
    z_far = (z + 2) % 4
    dev_up = {"dp": z_up * 4 + rest}
    dev_down = {"dp": z_down * 4 + rest}
    dev_far = {"dp": z_far * 4 + rest}
    dev_core = {"dp": d + 1 - 2 * core}
    dev_row = {"dp": z * 4 + (rest + 2) % 4}

    late = s < last - 2

    def w_copy(j):
        cols = pl.ds(pl.multiple_of(j * block, block), block)
        return pltpu.make_async_copy(w_hbm.at[0, :, cols], w_v.at[:, cols], sem_w.at[j])

    @pl.when(s == 0)
    def _():
        pltpu.make_async_copy(inputs_hbm, base_v, sem_base).start()

    @pl.when(has_prev)
    def _():
        pltpu.make_async_copy(stored_hbm.at[0, 0], base_v, sem_base).start()

    pltpu.make_async_copy(stored_hbm.at[0, 1], keep_v, sem_keep).start()
    for j in range(FIRST_COLUMNS):
        w_copy(j).start()

    barrier = pltpu.get_barrier_semaphore()

    @pl.when(has_next)
    def _():
        pl.semaphore_signal(barrier, inc=1, device_id=nxt, device_id_type=MESH)

    @pl.when(has_prev)
    def _():
        pl.semaphore_signal(barrier, inc=1, device_id=prv, device_id_type=MESH)

    for peer in (dev_up, dev_down, dev_far, dev_core, dev_row):
        pl.semaphore_signal(barrier, inc=1, device_id=peer, device_id_type=MESH)
    pl.semaphore_wait(barrier, 5 + jnp.minimum(s, 1) + jnp.minimum(last - s, 1))

    @pl.when(s == 0)
    def _():
        fin_v[...] = jnp.zeros_like(fin_v)

    pltpu.make_async_copy(inputs_hbm, base_v, sem_base).wait()
    for j in range(FIRST_COLUMNS, PIECES):
        w_copy(j).start()
    def prepare():
        side = 256
        line = lax.broadcasted_iota(jnp.int32, (side, side), 0)
        column = lax.broadcasted_iota(jnp.int32, (side, side), 1)
        eye = jnp.where(line == column, 1.0, 0.0).astype(bf16)

        def turn(i, carry):
            cols = pl.ds(pl.multiple_of(i * side, side), side)
            for j in range(PIECES):
                part = pl.ds(j * block, block)
                wt_v[cols, part] = lax.dot_general(
                    eye, w_v[part, cols], (((1,), (1,)), ((), ())), preferred_element_type=f32).astype(bf16)
            return carry

        lax.fori_loop(0, width // side, turn, 0)
        high = gain_ref[...].astype(bf16)
        low = (gain_ref[...] - high.astype(f32)).astype(bf16)
        which = lax.broadcasted_iota(jnp.int32, (16, width), 0)
        pair = jnp.where(which == 0, high.astype(f32), jnp.where(which == 1, low.astype(f32), 0.0)).astype(bf16)

        def weigh(j, carry):
            cols = pl.ds(pl.multiple_of(j * block, block), block)
            both = jnp.dot(pair, w_v[:, cols], preferred_element_type=f32)
            u_v[:, cols] = jnp.broadcast_to(jnp.sum(both, axis=0, keepdims=True), (8, block))
            return carry

        lax.fori_loop(0, PIECES, weigh, 0)

    @pl.when(s == 0)
    def _():
        u_v[...] = jnp.zeros_like(u_v)

    @pl.when(jnp.logical_not(late))
    def _():
        for j in range(PIECES):
            w_copy(j).wait()
        prepare()

    pltpu.make_async_copy(stored_hbm.at[0, 1], keep_v, sem_keep).wait()

    def remote(src, dst, send, recv, device):
        return pltpu.make_async_remote_copy(
            src_ref=src, dst_ref=dst, send_sem=send, recv_sem=recv, device_id=device, device_id_type=MESH)

    def cols_of(j):
        return pl.ds(pl.multiple_of(j * block, block), block)

    def fcopy(c, cols):
        return remote(clip_v.at[c, :, cols], fin_v.at[c, :, cols], fsend.at[c], frecv.at[c], nxt)

    def fwhole(c):
        return remote(clip_v.at[c], fin_v.at[c], fsend.at[c], frecv.at[c], nxt)

    def bcopy(c, j):
        cols = cols_of(j)
        return remote(clip_v.at[c, :, cols], bin_v.at[c, :, cols], bsend.at[c, j], brecv.at[c, j], prv)

    def place(c):
        batch = c // per_batch
        first = pl.multiple_of((c % per_batch) * rows, rows)
        sample = ids_ref[0, batch]
        index = jnp.where(s == 0, batch, sample)
        return batch, first, sample, index

    share = width // 4
    part = share // 4
    unit = width // 12
    split = unit * Z_UNITS
    low_lanes = pl.ds(0, split)
    high_lanes = pl.ds(split, width - split)

    def chunk_rows(c, n=1):
        return pl.ds(pl.multiple_of(c * rows, rows), n * rows)

    circle = ((0, z_up, dev_up), (1, z_down, dev_down), (2, z_far, dev_far))

    def z_copy(c, slot):
        return remote(gown_v.at[chunk_rows(c), low_lanes],
                      gz_v.at[pl.ds(pl.multiple_of(slot * local + c * rows, rows), rows)],
                      zsend.at[slot, c], zrecv.at[slot, c], circle[slot][2])

    def g_copy(c):
        return remote(gown_v.at[chunk_rows(c), high_lanes], gy_v.at[chunk_rows(c)], gsend.at[c], grecv.at[c], dev_row)

    def ncopy(slot):
        return remote(nt_v.at[circle[slot][1]],
                      ngat_v.at[:, pl.ds((slot + 1) * local, local)], nsend.at[slot], nrecv.at[slot], circle[slot][2])

    def nrow_copy():
        return remote(nt_v.at[:, pl.ds(pl.multiple_of((1 - row) * 2 * part, 2 * part), 2 * part)], nrow_v,
                      nsend.at[3], nrecv.at[3], dev_row)

    def share_normed():
        step = share // 3
        def turn(i, carry):
            cols = pl.ds(pl.multiple_of(i * step, step), step)
            for b in range(batches):
                values = normed_v[pl.ds(b * per_batch, per_batch), :, cols].reshape(tokens, step)
                nt_v[i // 3, pl.ds(pl.multiple_of((i % 3) * step, step), step), pl.ds(b * tokens, tokens)] = values.T
            return carry
        lax.fori_loop(0, width // step, turn, 0)
        for slot in range(3):
            ncopy(slot).start()
        nrow_copy().start()
        ngat_v[:, pl.ds(0, local)] = nt_v[z]

    def several(ref, c, n, cols=None):
        if cols is None:
            return ref[pl.ds(c, n)].reshape(n * rows, ref.shape[-1])
        return ref[pl.ds(c, n), :, cols].reshape(n * rows, cols.size)

    def keep(ref, c, n, value, cols=None):
        if cols is None:
            ref[pl.ds(c, n)] = value.reshape(n, rows, value.shape[-1])
        else:
            ref[pl.ds(c, n), :, cols] = value.reshape(n, rows, cols.size)

    def state_of(c, n, cols=None):
        batch, first, sample, index = place(c)
        if cols is None:
            return base_v[index, pl.ds(first, n * rows), :].astype(f32) + several(fin_v, c, n).astype(f32)
        return base_v[index, pl.ds(first, n * rows), cols].astype(f32) + several(fin_v, c, n, cols).astype(f32)

    def forward(c, n, final):
        batch, first, sample, index = place(c)
        if final:
            for i in range(n):
                fwhole(c + i).wait_recv()
        else:
            @pl.when(has_prev)
            def _():
                fwhole(c).wait_recv()

        x = state_of(c, n)
        mu = jnp.mean(x, axis=-1, keepdims=True)
        xc = x - mu
        var = jnp.mean(xc * xc, axis=-1, keepdims=True)
        rs = lax.rsqrt(var + epsilon)
        keep(normed_v, c, n, (xc * rs * gain_ref[...]).astype(bf16))
        keep(mu_v, c, n, jnp.broadcast_to(mu, (n * rows, 128)))
        keep(rs_v, c, n, jnp.broadcast_to(rs, (n * rows, 128)))

        pieces = FINAL_PIECES if final else PIECES
        narrow = width // pieces

        def tile(j, carry2):
            cols = pl.ds(pl.multiple_of(j * narrow, narrow), narrow)
            if not final:
                @pl.when(jnp.logical_and(c == 0, late))
                def _():
                    w_copy(j).wait()

            v = jnp.dot(several(normed_v, c, n), w_v[:, cols], preferred_element_type=f32)
            cdf = 0.5 + 0.5 * lax.erf(v * rsqrt2)
            res = state_of(c, n, cols) + v * cdf
            out_v[batch, pl.ds(first, n * rows), cols] = res.astype(bf16)
            if not final:
                kept = keep_v[sample, pl.ds(first, rows), cols].astype(f32)
                clip_v[c, :, cols] = jnp.clip(res - kept, -delta_bound, delta_bound).astype(bf16)
                fcopy(c, cols).start()
                keep(pre_v, c, n, v, cols)
            slope = cdf + v * (jnp.exp(-0.5 * v * v) * rsqrt2pi)
            if not final:
                keep(slope_v, c, n, slope.astype(bf16), cols)
                return carry2
            up = res * scale
            keep(pre_v, 0, n, up, cols)
            return push_back(c, n, cols, slope * up, v, carry2)

        zero = jnp.zeros((n * rows, 1), f32)
        sums = lax.fori_loop(0, pieces, tile, (zero, zero) if final else 0)
        return sums

    def push_back(c, n, cols, value, v, sums):
        gp = value.astype(bf16)
        gown_v[chunk_rows(c, n), cols] = gp
        wide_gp = gp.astype(f32)
        return (
            sums[0] + jnp.sum(wide_gp * u_v[0:1, cols], axis=-1, keepdims=True),
            sums[1] + jnp.sum(wide_gp * v, axis=-1, keepdims=True),
        )

    def backward(c, n, sums):
        final = sums is not None

        def piece(j, sums):
            cols = cols_of(j)
            bcopy(c, j).wait_recv()
            up = several(bin_v, c, n, cols).astype(f32)
            return push_back(c, n, cols, several(slope_v, c, n, cols).astype(f32) * up, several(pre_v, c, n, cols), sums)

        if not final:
            zero = jnp.zeros((n * rows, 1), f32)
            sums = lax.fori_loop(0, PIECES, piece, (zero, zero))
        for i in range(n):
            for slot in range(3):
                z_copy(c + i, slot).start()

        if not final:
            @pl.when(s == 0)
            def _():
                g_copy(c).start()

        def pull():
            m1 = sums[0] * (1.0 / width)
            m2 = sums[1] * (1.0 / width)
            mu = several(mu_v, c, n)[:, :1]
            rs = several(rs_v, c, n)[:, :1]
            if not final:
                fwhole(c).wait_send()

            def tile(j, carry2):
                cols = cols_of(j)
                gn = jnp.dot(gown_v[chunk_rows(c, n)], wt_v[:, cols], preferred_element_type=f32)
                state = state_of(c, n, cols)
                xhat = (state - mu) * rs
                if final:
                    up = several(pre_v, 0, n, cols)
                else:
                    up = several(bin_v, c, n, cols).astype(f32)
                sent = up + rs * (gn * gain_ref[:, cols] - m1 - xhat * m2)
                keep(clip_v, c, n, sent.astype(bf16), cols)
                bcopy(c, j).start()
                return carry2

            lax.fori_loop(0, PIECES, tile, 0)
            for i in range(1, n):
                for j in range(PIECES):
                    bcopy(c + i, j).start()

        if final:
            pull()
        else:
            pl.when(has_prev)(pull)

    def forward_step(c, carry):
        forward(c, 1, False)
        return carry

    def backward_step(c, carry):
        backward(c, 1, None)
        return carry

    def pair_step(t, carry):
        sums = forward(2 * t, 2, True)

        backward(2 * t, 2, sums)
        return carry

    @pl.when(has_next)
    def _():
        lax.fori_loop(0, chunks, forward_step, 0)

        @pl.when(late)
        def _():
            share_normed()

            @pl.when(has_prev)
            def _():
                prepare()

        lax.fori_loop(0, chunks, backward_step, 0)

    @pl.when(s == last)
    def _():
        lax.fori_loop(0, chunks // 2, pair_step, 0)

    for peer in (dev_up, dev_down, dev_far, dev_core, dev_row):
        pl.semaphore_signal(ready, inc=1, device_id=peer, device_id_type=MESH)

    def start_rows(c, carry):
        g_copy(c).start()
        return carry

    @pl.when(has_prev)
    def _():
        lax.fori_loop(0, chunks, start_rows, 0)

    @pl.when(jnp.logical_not(late))
    def _():
        share_normed()

    def band(place_of, lanes, count=1):
        return (pl.ds(place_of * part, count * part), lanes)

    def lanes_of(q):
        return pl.ds(pl.multiple_of(q * unit, unit), unit)

    def core_copy(q, y):
        lanes = lanes_of(q)
        return remote(w_v.at[band(y, lanes)], wt_v.at[band(y, lanes)], csend.at[q, y], crecv.at[q, y], dev_core)

    def row_copy(q):
        lanes = lanes_of(q)
        return remote(w_v.at[band(4, lanes)], wt_v.at[band(2, lanes)], ysend.at[q], yrecv.at[q], dev_row)

    def core_copy2(q):
        lanes = lanes_of(q)
        return remote(w_v.at[band(6, lanes, 4)], wt_v.at[band(3, lanes, 4)], csend2.at[q], crecv2.at[q], dev_core)

    def sum_rows(z_of):
        return pl.ds(pl.multiple_of((10 + z_of) * part, part), part)

    def far_half(q, side):
        lanes = lanes_of(q)
        lines = pl.ds(pl.multiple_of((10 + z_far) * part + side * (part // 2), part // 2), part // 2)
        return remote(w_v.at[lines, lanes], wt_v.at[pl.ds(7 * part + side * (part // 2), part // 2), lanes],
                      zsend2.at[side, q], zrecv2.at[side, q], circle[side][2])

    def near_block(q, side):
        lanes = lanes_of(q)
        return remote(w_v.at[sum_rows(circle[side][1]), lanes], wt_v.at[band(8 + side, lanes)],
                      zsend2.at[2 + side, q], zrecv2.at[2 + side, q], circle[side][2])

    def came(c, carry):
        g_copy(c).wait_recv()
        return carry

    pl.semaphore_wait(ready, 5)

    def high_product(whose, lanes, high):
        mine = nt_v[:, pl.ds(pl.multiple_of(row * 2 * part + whose * part, part), part)].reshape(share, local)
        theirs = nrow_v[:, pl.ds(pl.multiple_of(whose * part, part), part)].reshape(share, local)
        return (
            jnp.dot(mine, gown_v[:, lanes], preferred_element_type=f32)
            + jnp.dot(theirs, gy_v[:, high], preferred_element_type=f32)
        ).astype(bf16)

    def product2(q):
        lanes = lanes_of(q)
        high = pl.ds(pl.multiple_of((q - Z_UNITS) * unit, unit), unit)
        w_v[band(6, lanes, 4)] = high_product(1 - core, lanes, high)
        core_copy2(q).start()
        w_v[band(10, lanes, 4)] = high_product(core, lanes, high)

    def pair_sum2(q):
        lanes = lanes_of(q)
        core_copy2(q).wait_recv()
        w_v[band(10, lanes, 4)] = (
            w_v[band(10, lanes, 4)].astype(f32) + wt_v[band(3, lanes, 4)].astype(f32)
        ).astype(bf16)
        for side in range(2):
            far_half(q, side).start()

    def near_sum2(q):
        lanes = lanes_of(q)
        for side in range(2):
            far_half(q, side).wait_recv()
            lines = pl.ds(pl.multiple_of((10 + circle[side][1]) * part + side * (part // 2), part // 2), part // 2)
            w_v[lines, lanes] = (
                w_v[lines, lanes].astype(f32)
                + wt_v[pl.ds(7 * part + side * (part // 2), part // 2), lanes].astype(f32)
            ).astype(bf16)
            near_block(q, side).start()

    def arrived(c, carry):
        for slot in range(3):
            z_copy(c, slot).wait_recv()
        return carry

    def low_product(y, whose, lanes):
        lines = pl.ds(pl.multiple_of(y * 2 * part + whose * part, part), part)
        return (
            jnp.dot(ngat_v[lines, pl.ds(0, local)], gown_v[:, lanes], preferred_element_type=f32)
            + jnp.dot(ngat_v[lines, pl.ds(local, 3 * local)], gz_v[:, lanes], preferred_element_type=f32)
        ).astype(bf16)

    def one_of(first, which):
        return pl.ds(pl.multiple_of((first + which) * part, part), part)

    def product(q):
        lanes = lanes_of(q)
        for y in range(2):
            w_v[band(y, lanes)] = low_product(y, 1 - core, lanes)
            core_copy(q, y).start()
        for y in range(2):
            w_v[band(2 + y, lanes)] = low_product(y, core, lanes)

    def pair_sum(q):
        lanes = lanes_of(q)
        for y in range(2):
            core_copy(q, y).wait_recv()
        w_v[band(4, lanes)] = (
            w_v[one_of(2, 1 - row), lanes].astype(f32) + wt_v[one_of(0, 1 - row), lanes].astype(f32)
        ).astype(bf16)
        row_copy(q).start()

    high_units = 12 - Z_UNITS
    high_first = jnp.where(s == 0, 0, Z_UNITS)
    low_first = jnp.where(s == 0, high_units, 0)
    near_lag = jnp.where(s == 0, NEAR_LAG, 2)

    def tail(t, carry):
        def at(begin, count, work, shift):
            @pl.when(jnp.logical_and(t >= begin, t < begin + count))
            def _():
                work(t - begin + shift)

        @pl.when(t == high_first)
        def _():
            nrow_copy().wait_recv()
            lax.fori_loop(0, chunks, came, 0)

        at(high_first, high_units, product2, Z_UNITS)
        at(high_first + LAG, high_units, pair_sum2, Z_UNITS)

        @pl.when(t == low_first)
        def _():
            for slot in range(3):
                ncopy(slot).wait_recv()
            lax.fori_loop(0, chunks, arrived, 0)

        at(low_first, Z_UNITS, product, 0)
        at(low_first + LAG, Z_UNITS, pair_sum, 0)
        at(high_first + LAG + near_lag, high_units, near_sum2, Z_UNITS)
        return carry

    lax.fori_loop(0, jnp.where(s == 0, max(12 + LAG, LAG + NEAR_LAG + high_units), 12 + LAG + 2), tail, 0)

    def total2(q, carry):
        lanes = lanes_of(q)
        result = w_v[sum_rows(z), lanes].astype(f32)
        for side in range(2):
            near_block(q, side).wait_recv()
            result += wt_v[band(8 + side, lanes)].astype(f32)
        wgrad_v[:, lanes] = result.astype(bf16)
        return carry

    def total(q, carry):
        lanes = lanes_of(q)
        row_copy(q).wait_recv()
        wgrad_v[:, lanes] = (
            w_v[one_of(2, row), lanes].astype(f32) + wt_v[one_of(0, row), lanes].astype(f32)
            + wt_v[band(2, lanes)].astype(f32)
        ).astype(bf16)
        return carry

    def totals(t, carry):
        q = (t + jnp.where(s == 0, Z_UNITS, 0)) % 12

        @pl.when(q < Z_UNITS)
        def _():
            total(q, 0)

        @pl.when(q >= Z_UNITS)
        def _():
            total2(q, 0)

        return carry

    lax.fori_loop(0, 12, totals, 0)

    def finish(c, carry):
        g_copy(c).wait_send()
        for slot in range(3):
            z_copy(c, slot).wait_send()

        @pl.when(s == 0)
        def _():
            fwhole(c).wait_send()

        @pl.when(has_prev)
        def _():
            for j in range(PIECES):
                bcopy(c, j).wait_send()

        return carry

    lax.fori_loop(0, chunks, finish, 0)

    def finish_low(q, carry):
        for y in range(2):
            core_copy(q, y).wait_send()
        row_copy(q).wait_send()
        return carry

    def finish_high(q, carry):
        core_copy2(q).wait_send()
        for side in range(2):
            far_half(q, side).wait_send()
            near_block(q, side).wait_send()
        return carry

    lax.fori_loop(0, Z_UNITS, finish_low, 0)
    lax.fori_loop(Z_UNITS, 12, finish_high, 0)
    for slot in range(3):
        ncopy(slot).wait_send()
    nrow_copy().wait_send()


def relay(scale, inputs, sample_ids, stored, weight, norm_gain):
    batches, tokens, width = inputs.shape
    rows = min(CHUNK, tokens)
    local = batches * tokens
    chunks = local // rows
    share = width // 4
    part = share // 4
    split = width // 12 * Z_UNITS
    any_spec = pl.BlockSpec(memory_space=pl.ANY)
    chunked = pltpu.VMEM((chunks, rows, width), bf16)
    dma = pltpu.SemaphoreType.DMA
    return pl.pallas_call(
        functools.partial(relay_kernel, scale),
        out_shape=(
            pltpu.VMEM(inputs.shape, bf16),
            pltpu.VMEM((part, width), bf16),
        ),
        in_specs=[
            pl.BlockSpec(memory_space=pltpu.SMEM), any_spec, any_spec, any_spec,
            pl.BlockSpec(memory_space=pltpu.VMEM),
        ],
        out_specs=(pl.BlockSpec(memory_space=pltpu.VMEM), pl.BlockSpec(memory_space=pltpu.VMEM)),
        scratch_shapes=[
            pltpu.VMEM((width, width), bf16),
            pltpu.VMEM((width, width), bf16),
            pltpu.VMEM(inputs.shape, bf16),
            pltpu.VMEM(inputs.shape, bf16),
            chunked, chunked, chunked,
            pltpu.VMEM((chunks, rows, width), f32),
            chunked, chunked,
            pltpu.VMEM((chunks, rows, 128), f32),
            pltpu.VMEM((chunks, rows, 128), f32),
            pltpu.VMEM((8, width), f32),
            pltpu.VMEM((4, share, local), bf16),
            pltpu.VMEM((share, 4 * local), bf16),
            pltpu.VMEM((4, 2 * part, local), bf16),
            pltpu.VMEM((local, width), bf16),
            pltpu.VMEM((3 * local, split), bf16),
            pltpu.VMEM((local, width - split), bf16),
            dma((PIECES,)), dma, dma,
            dma((chunks,)), dma((chunks,)),
            dma((chunks, PIECES)), dma((chunks, PIECES)),
            dma((4,)), dma((4,)),
            dma((3, chunks)), dma((3, chunks)),
            dma((chunks,)), dma((chunks,)),
            dma((Z_UNITS, 2)), dma((Z_UNITS, 2)),
            dma((Z_UNITS,)), dma((Z_UNITS,)),
            dma((12,)), dma((12,)),
            dma((4, 12)), dma((4, 12)),
            pltpu.SemaphoreType.REGULAR,
        ],
        compiler_params=pltpu.CompilerParams(
            collective_id=0, has_side_effects=True, vmem_limit_bytes=VMEM_LIMIT),
        cost_estimate=pl.CostEstimate(
            flops=6 * local * width * width, bytes_accessed=2 * width * width, transcendentals=0),
        name="relay",
    )(sample_ids, inputs, stored, weight, norm_gain)


def per_device(inputs, sample_ids, stored, weight, norm_gain):
    batches, tokens, width = inputs.shape
    scale = 1.0 / math.sqrt(lax.axis_size("dp") * batches * tokens)
    outs, summed = relay(scale, inputs, sample_ids, stored, weight, norm_gain)
    return (outs[None], summed[None])


def solution(mesh):
    return jax.shard_map(
        per_device,
        mesh=mesh,
        in_specs=(
            P("dp", None, None),
            P("dp", None),
            P("section", None, "dp", None, None),
            P("section", None, None),
            P("section", None),
        ),
        out_specs=(P("section", "dp", None, None), P("section", "dp", None)),
        check_vma=False,
    )
```
